1024 devices in a mesh: batch: 64 (over y_hi, x, core), seq: 16 (over z, y_lo).
Axes of the slice: x: 8, y: 8 (y_hi: 4, y_lo: 2; y = y_hi * 2 + y_lo), z: 8, core: 2. Of those that a mesh axis runs over, the one named last changes fastest.
Arguments:
- queries: bfloat16 [64, 2048, 1280], P('batch', 'seq'), may hold values from -120 to 120
- keys: bfloat16 [64, 2048, 1280], P('batch', 'seq'), may hold values from -7.5 to 7.5
- values: bfloat16 [64, 2048, 1280], P('batch', 'seq'), may hold values from -6 to 6
- residual_in: bfloat16 [64, 2048, 1280], P('batch', 'seq'), may hold values from -3 to 3
- w_out: bfloat16 [1280, 1280], replicated, may hold values from -0.15625 to 0.15625
- ln_gain: float32 [1280], replicated, may hold values from 0.5 to 1.5
- w_proj: bfloat16 [1280, 1024], replicated, may hold values from -0.15625 to 0.15625
- texts: float32 [64, 1024], P('batch', 'seq'), may hold values from -1200 to 1200
- labels: int32 [64], replicated, may hold values from 0 to 63, each once
Outputs:
- hidden_out: bfloat16 [64, 2048, 1280], P('batch', 'seq')
- image_loss: float32 [64], P('batch')
- text_loss: float32 [64], P('batch')
The draws below stay inside these ranges and needn't reach their ends.
All inputs are finite; a program needn't handle non-finite values.
Results may differ from the reference program's by a relative error of at most 0.0034.
Values may be sent and summed in bfloat16 or wider, within the bound.
A program may use at most 32 MiB of HBM per device.

```python
import jax
import jax.numpy as jnp
from jax import lax

D = 1280
HEADS = 16
HEAD_DIM = 80
EMBED = 1024
PATCHES = 2048
IMAGES = 64
TEXTS = 64


def drawn_pair(key):
    key_query, key_key = jax.random.split(jax.random.fold_in(key, 7), 2)
    shape = (IMAGES, PATCHES, D)
    query_draw = 1.5 * jnp.clip(jax.random.normal(key_query, shape, jnp.float32), -5.0, 5.0)
    key_draw = 1.5 * jnp.clip(jax.random.normal(key_key, shape, jnp.float32), -5.0, 5.0)
    return (query_draw, key_draw)


def draw_queries(key, part):
    return drawn_pair(key)[0].astype(jnp.bfloat16)


def draw_keys(key, part):
    return drawn_pair(key)[1].astype(jnp.bfloat16)


def draw_texts(key, part):
    key_base, key_scale = jax.random.split(jax.random.fold_in(key, 11), 2)
    base = jnp.clip(jax.random.normal(key_base, (TEXTS, EMBED), jnp.float32), -4.5, 4.5)
    scales = jnp.exp(jax.random.uniform(key_scale, (TEXTS, 1), jnp.float32, jnp.log(2.0), jnp.log(20.0)))
    result = base * scales
    return result


def level_of(stream_key, extent, pieces, low, high):
    gain = 1.0
    for axis_at, shards_of in pieces:
        draws = jax.random.uniform(jax.random.fold_in(jax.random.fold_in(stream_key, 6), axis_at), (shards_of,), jnp.float32, low / len(pieces), high / len(pieces))
        gain = gain * jnp.repeat(jnp.exp(draws), extent[axis_at] // shards_of).reshape((-1,) + (1,) * (len(extent) - 1 - axis_at))
    return gain


def scatter_about(stream_key, shape, width, bound, shards=(), kind=jnp.bfloat16):
    values = width * jax.random.normal(stream_key, shape, jnp.float32)
    if shards:
        values = values * level_of(stream_key, shape, shards, -0.22, 0.18)
    return jnp.clip(values, -bound, bound).astype(kind)


def setup_inputs(seed: int = 0) -> dict:
    key_list = jax.random.split(jax.random.key(seed), 10)
    queries = draw_queries(jax.random.fold_in(key_list[9], 71), 0)
    keys = draw_keys(jax.random.fold_in(key_list[9], 71), 0)
    values = scatter_about(key_list[2], (IMAGES, PATCHES, D), 1.0, 6.0, ((0, 64), (1, 16)))
    residual_in = scatter_about(key_list[3], (IMAGES, PATCHES, D), 0.5, 3.0, ((0, 64), (1, 16)))
    w_out = scatter_about(key_list[4], (D, D), D ** -0.5, 0.15625)
    ln_gain = jnp.clip(1.0 + 0.1 * jax.random.normal(key_list[5], (D,), jnp.float32), 0.5, 1.5)
    w_proj = scatter_about(key_list[6], (D, EMBED), D ** -0.5, 0.15625)
    texts = draw_texts(jax.random.fold_in(key_list[9], 71), 0)
    labels = jax.random.permutation(key_list[8], TEXTS).astype(jnp.int32)
    return dict(queries=queries, keys=keys, values=values, residual_in=residual_in, w_out=w_out, ln_gain=ln_gain, w_proj=w_proj, texts=texts, labels=labels)


def attend_image(operands):
    query_rows, key_rows, value_rows = operands
    block_rows = min(512, PATCHES)
    query_heads = query_rows.astype(jnp.float32).reshape(PATCHES, HEADS, HEAD_DIM)
    key_heads = key_rows.astype(jnp.float32).reshape(PATCHES, HEADS, HEAD_DIM)
    value_heads = value_rows.astype(jnp.float32).reshape(PATCHES, HEADS, HEAD_DIM)
    score_scale = HEAD_DIM ** (-0.5)

    def one_block(offset):
        query_block = lax.dynamic_slice_in_dim(query_heads, offset, block_rows, 0)
        scores = jnp.einsum('qhd,khd->hqk', query_block, key_heads) * score_scale
        maxima = lax.optimization_barrier(jnp.max(scores, axis=-1, keepdims=True))
        weights = jnp.exp(scores - maxima)
        weights = (weights / lax.optimization_barrier(jnp.sum(weights, axis=-1, keepdims=True))).astype(jnp.bfloat16)
        weights = lax.optimization_barrier(weights)
        mixed = jnp.einsum('hqk,khd->qhd', weights.astype(jnp.float32), value_heads)
        return mixed.astype(jnp.bfloat16).reshape(block_rows, D)
    offsets = (jnp.arange(PATCHES // block_rows) * block_rows).astype(jnp.int32)
    return lax.map(one_block, offsets).reshape(PATCHES, D)

def row_lse(logits, axis):
    maxima = lax.optimization_barrier(jnp.max(logits, axis=axis, keepdims=True))
    return jnp.squeeze(maxima, axis) + jnp.log(lax.optimization_barrier(jnp.sum(jnp.exp(logits - maxima), axis=axis)))

def contrastive(logits, labels):
    matched = labels[:, None] == jnp.arange(logits.shape[1], dtype=jnp.int32)[None, :]
    picked = jnp.where(matched, logits, jnp.float32(0.0))
    image_loss = row_lse(logits, 1) - lax.optimization_barrier(jnp.sum(picked, axis=1))
    text_loss = row_lse(logits, 0) - lax.optimization_barrier(jnp.sum(picked, axis=0))
    return (image_loss, text_loss)

def reference(queries, keys, values, residual_in, w_out, ln_gain, w_proj, texts, labels):
    attended = lax.map(attend_image, (queries, keys, values))
    mixed_out = jnp.dot(attended.reshape(-1, D), w_out, preferred_element_type=jnp.float32)
    summed = residual_in.astype(jnp.float32) + mixed_out.reshape(IMAGES, PATCHES, D)
    hidden_out = summed.astype(jnp.bfloat16)
    centred = summed - lax.optimization_barrier(jnp.mean(summed, axis=-1, keepdims=True))
    variance = lax.optimization_barrier(jnp.mean(centred * centred, axis=-1, keepdims=True))
    normed = centred * lax.rsqrt(variance + 1e-05) * ln_gain
    pooled = lax.optimization_barrier(jnp.mean(normed, axis=1))
    embedding = jnp.dot(pooled, w_proj.astype(jnp.float32), precision=lax.Precision.HIGHEST)
    inverse = lax.rsqrt(lax.optimization_barrier(jnp.sum(embedding * embedding, axis=1)) + 1e-06)
    logits = jnp.dot(embedding * inverse[:, None], texts.T, precision=lax.Precision.HIGHEST)
    image_loss, text_loss = contrastive(logits, labels)
    return (hidden_out, image_loss, text_loss)
```

```python
import math

import jax
import jax.numpy as jnp
from jax import lax
from jax.experimental import pallas as pl
from jax.experimental.pallas import tpu as pltpu
from jax.sharding import PartitionSpec as P

HEADS = 16
HD = 80
D = 1280
EMBED = 1024
PATCHES = 2048
ROWS = 128
NSEQ = 16
NZ = 8
NB = 64
NB1 = 16
NB2 = 4
CHUNK = 2 * ROWS
KB = 256
MESH = pl.DeviceIdType.MESH
F32 = jnp.float32
BF16 = jnp.bfloat16


def depth_step(t):
    half = (t + 1) // 2
    return lax.rem(4 + half * (1 - 2 * lax.rem(t, 2)) + NZ, NZ)


def kernel(
    q_hbm, k_hbm, v_hbm, res_hbm, wout_hbm, gain_ref, wproj_hbm, texts_ref, labels_ref,
    hid_hbm, img_ref, txt_ref,
    q_in, k_in, v_in, res_in, wout, wproj, hid,
    kv_send, q_send, kv_recv, q_recv, o_send, o_recv,
    k_all, vt_all, s_all, acc, t0, tex, e_buf, rows,
    load_sem, kv_ss, kv_rs, q_ss, q_rs, o_ss, o_rs, t0_ss, t0_rs, t1_ss, t1_rs, t2_ss, t2_rs,
    e_ss, e_rs, b1_ss, b1_rs, b2_ss, b2_rs,
):
    b = lax.axis_index("batch")
    s = lax.axis_index("seq")
    z, y = s // 2, lax.rem(s, 2)
    b_hi, b_lo = b // NB1, lax.rem(b, NB1)

    loads = [
        pltpu.make_async_copy(src, dst, load_sem.at[i])
        for i, (src, dst) in enumerate(
            [(k_hbm, k_in), (v_hbm, v_in), (q_hbm, q_in), (res_hbm, res_in), (wout_hbm, wout), (wproj_hbm, wproj)]
        )
    ]
    for load in loads[:4]:
        load.start()

    barrier = pltpu.get_barrier_semaphore()

    def greet_seq(r, c):
        pl.semaphore_signal(barrier, inc=1, device_id=(b, lax.rem(s + r, NSEQ)), device_id_type=MESH)
        pl.semaphore_signal(
            barrier, inc=1, device_id=(b_hi * NB1 + lax.rem(b_lo + r, NB1), s), device_id_type=MESH
        )
        return c

    lax.fori_loop(1, NSEQ, greet_seq, 0)

    def greet_far(r, c):
        pl.semaphore_signal(barrier, inc=1, device_id=(lax.rem(b + r * NB1, NB), s), device_id_type=MESH)
        return c

    lax.fori_loop(1, NB2, greet_far, 0)

    def turn(src, put):
        for c in range(D // 128):
            block = src[:, c * 128 : (c + 1) * 128].T
            i = 0
            while i < 8:
                g = c * 8 + i
                n = min(8 - i, 5 - g % 5)
                put(g // 5, (g % 5) * 16, block[i * 16 : (i + n) * 16], n * 16)
                i += n

    def put_k(h, r, value, n):
        kv_send[h, r : r + n, :] = value

    def put_v(h, r, value, n):
        kv_send[h, HD + r : HD + r + n, :] = value

    def put_q(h, r, value, n):
        q_send[h, r : r + n, :] = value

    loads[0].wait()
    turn(k_in, put_k)
    loads[1].wait()
    turn(v_in, put_v)
    loads[4].start()
    loads[5].start()

    piece = texts_ref[...]
    blank = jnp.zeros((1, 64), F32)
    even = jnp.concatenate([piece, blank], axis=1)
    odd = jnp.concatenate([blank, piece], axis=1)
    t0[s] = jnp.where(y == 0, even, odd)

    pl.semaphore_wait(barrier, 2 * (NSEQ - 1) + NB2 - 1)

    def kv_copy(to, frm):
        return pltpu.make_async_remote_copy(
            src_ref=kv_send.at[to], dst_ref=kv_recv.at[frm], send_sem=kv_ss.at[to], recv_sem=kv_rs.at[frm],
            device_id=(b, to), device_id_type=MESH,
        )

    def q_copy(to, frm):
        return pltpu.make_async_remote_copy(
            src_ref=q_send.at[to], dst_ref=q_recv.at[frm], send_sem=q_ss.at[to], recv_sem=q_rs.at[frm],
            device_id=(b, to), device_id_type=MESH,
        )

    def o_copy(to, frm):
        return pltpu.make_async_remote_copy(
            src_ref=o_send.at[to], dst_ref=o_recv.at[frm], send_sem=o_ss.at[to], recv_sem=o_rs.at[frm],
            device_id=(b, to), device_id_type=MESH,
        )

    def t0_copy(to, frm):
        return pltpu.make_async_remote_copy(
            src_ref=t0.at[frm], dst_ref=t0.at[frm], send_sem=t0_ss.at[to], recv_sem=t0_rs.at[frm],
            device_id=(b, to), device_id_type=MESH,
        )

    def e_copy(to, frm):
        return pltpu.make_async_remote_copy(
            src_ref=e_buf.at[frm], dst_ref=e_buf.at[frm], send_sem=e_ss.at[to], recv_sem=e_rs.at[frm],
            device_id=(b, to), device_id_type=MESH,
        )

    def t1_copy(to, frm):
        at = b_hi * NB1 + frm
        return pltpu.make_async_remote_copy(
            src_ref=tex.at[at], dst_ref=tex.at[at], send_sem=t1_ss.at[to], recv_sem=t1_rs.at[frm],
            device_id=(b_hi * NB1 + to, s), device_id_type=MESH,
        )

    def b1_copy(to, frm):
        at = b_hi * NB1 + frm
        return pltpu.make_async_remote_copy(
            src_ref=rows.at[at], dst_ref=rows.at[at], send_sem=b1_ss.at[to], recv_sem=b1_rs.at[frm],
            device_id=(b_hi * NB1 + to, s), device_id_type=MESH,
        )

    def t2_copy(to, frm):
        at = pl.ds(frm * NB1, NB1)
        return pltpu.make_async_remote_copy(
            src_ref=tex.at[at], dst_ref=tex.at[at], send_sem=t2_ss.at[to], recv_sem=t2_rs.at[frm],
            device_id=(to * NB1 + b_lo, s), device_id_type=MESH,
        )

    def b2_copy(to, frm):
        at = pl.ds(frm * NB1, NB1)
        return pltpu.make_async_remote_copy(
            src_ref=rows.at[at], dst_ref=rows.at[at], send_sem=b2_ss.at[to], recv_sem=b2_rs.at[frm],
            device_id=(to * NB1 + b_lo, s), device_id_type=MESH,
        )

    def others(count, me, act):
        def step(r, c):
            act(lax.rem(me + r, count))
            return c

        lax.fori_loop(1, count, step, 0)

    def by_depth(sign, act):
        def step(t, c):
            there = lax.rem(z + sign * depth_step(t) + NZ, NZ)
            for w in range(2):
                peer = 2 * there + lax.rem(y + w, 2)

                @pl.when(peer != s)
                def _():
                    act(peer)

            return c

        lax.fori_loop(0, NZ, step, 0)

    by_depth(1, lambda p: kv_copy(p, s).start())
    others(NSEQ, s, lambda p: t0_copy(p, s).start())

    loads[2].wait()
    turn(q_in, put_q)
    by_depth(1, lambda p: q_copy(p, s).start())

    others(NSEQ, s, lambda p: t0_copy(s, p).wait_recv())
    for k in range(8):
        tex[b, k : k + 1, :] = t0[2 * k] + t0[2 * k + 1]
    others(NB1, b_lo, lambda p: t1_copy(p, b_lo).start())

    kv_recv[s] = kv_send[s]
    q_recv[s] = q_send[s]
    top = lax.broadcasted_iota(jnp.int32, (16, PATCHES), 0)
    vt_all[HD : HD + 16, :] = jnp.where(top == 0, 1.0, 0.0).astype(BF16)

    others(NB1, b_lo, lambda p: t1_copy(b_lo, p).wait_recv())
    others(NB2, b_hi, lambda p: t2_copy(p, b_hi).start())

    def take_kv(t, c):
        there = lax.rem(z - depth_step(t) + NZ, NZ)
        for w in range(2):
            peer = 2 * there + w

            @pl.when(peer != s)
            def _():
                kv_copy(s, peer).wait_recv()

            block = kv_recv[peer]
            k_all[pl.ds(pl.multiple_of((2 * t + w) * ROWS, ROWS), ROWS), :] = block[:HD].T
            vt_all[0:HD, pl.ds(pl.multiple_of((2 * t + w) * ROWS, ROWS), ROWS)] = block[HD:]
        return c

    lax.fori_loop(0, NZ, take_kv, 0)

    loads[3].wait()
    factor = HD ** (-0.5) * math.log2(math.e)

    def attend(t, c):
        there = lax.rem(z - depth_step(t) + NZ, NZ)
        for w in range(2):
            peer = 2 * there + w

            @pl.when(peer != s)
            def _():
                q_copy(s, peer).wait_recv()

        qt = jnp.concatenate([q_recv[2 * there], q_recv[2 * there + 1]], axis=1)
        top8 = None
        for i in range(PATCHES // KB):
            part = jnp.dot(k_all[i * KB : (i + 1) * KB, :], qt, preferred_element_type=F32)
            s_all[i * KB : (i + 1) * KB, :] = part
            high = jnp.max(part.reshape(KB // 8, 8, CHUNK), axis=0)
            top8 = high if top8 is None else jnp.maximum(top8, high)
        maxima = jnp.max(top8, axis=0, keepdims=True)
        total = None
        for i in range(PATCHES // KB):
            weights = jnp.exp2((s_all[i * KB : (i + 1) * KB, :] - maxima) * factor).astype(BF16)
            part = jnp.dot(vt_all[:, i * KB : (i + 1) * KB], weights, preferred_element_type=F32)
            total = part if total is None else total + part
        mixed = (total[:HD] / total[HD : HD + 1]).astype(BF16)
        for w in range(2):
            peer = 2 * there + w
            value = mixed[:, w * ROWS : (w + 1) * ROWS]

            @pl.when(peer != s)
            def _():
                o_send[peer] = value
                o_copy(peer, s).start()

            @pl.when(peer == s)
            def _():
                o_recv[s] = value

        return c

    lax.fori_loop(0, NZ, attend, 0)

    others(NSEQ, s, lambda p: kv_copy(p, s).wait_send())
    others(NSEQ, s, lambda p: q_copy(p, s).wait_send())
    others(NSEQ, s, lambda p: t0_copy(p, s).wait_send())
    others(NB1, b_lo, lambda p: t1_copy(p, b_lo).wait_send())
    others(NB2, b_hi, lambda p: t2_copy(p, b_hi).wait_send())
    others(NB2, b_hi, lambda p: t2_copy(b_hi, p).wait_recv())

    acc[...] = res_in[...].astype(F32)
    loads[4].wait()

    def project(t, c):
        there = lax.rem(z + depth_step(t) + NZ, NZ)
        for w in range(2):
            peer = 2 * there + w

            @pl.when(peer != s)
            def _():
                o_copy(s, peer).wait_recv()

        part = jnp.concatenate([o_recv[2 * there], o_recv[2 * there + 1]], axis=0).T
        weight = wout[pl.ds(pl.multiple_of(there * 2 * HD, 2 * HD), 2 * HD), :]
        acc[...] += jnp.dot(part, weight, preferred_element_type=F32)
        return c

    lax.fori_loop(0, NZ, project, 0)

    pool = None
    for i in range(ROWS // 16):
        x = acc[i * 16 : (i + 1) * 16, :]
        hid[i * 16 : (i + 1) * 16, :] = x.astype(BF16)
        centred = x - jnp.sum(x, axis=1, keepdims=True) * (1.0 / D)
        variance = jnp.sum(centred * centred, axis=1, keepdims=True) * (1.0 / D)
        normed = (centred * lax.rsqrt(variance + 1e-05)).reshape(2, 8, D)
        part = normed[0] + normed[1]
        pool = part if pool is None else pool + part
    hid_copy = pltpu.make_async_copy(hid, hid_hbm.at[0], load_sem.at[6])
    hid_copy.start()

    pooled = jnp.sum(pool, axis=0, keepdims=True) * gain_ref[...] * (1.0 / PATCHES)
    first = pooled.astype(BF16).astype(F32)
    rest = pooled - first
    second = rest.astype(BF16).astype(F32)
    third = rest - second
    at = lax.broadcasted_iota(jnp.int32, (16, D), 0)
    split = jnp.where(at == 0, first, jnp.where(at == 1, second, jnp.where(at == 2, third, 0.0))).astype(BF16)
    loads[5].wait()
    projected = jnp.sum(jnp.dot(split, wproj[...], preferred_element_type=F32)[0:8], axis=0, keepdims=True)
    for k in range(8):
        e_buf[s, k : k + 1, :] = projected[:, k * 128 : (k + 1) * 128]
    others(NSEQ, s, lambda p: e_copy(p, s).start())

    others(NSEQ, s, lambda p: o_copy(p, s).wait_send())
    label_row = labels_ref[...]
    lane64 = lax.broadcasted_iota(jnp.int32, (1, 64), 1)
    own_label = jnp.sum(jnp.where(lane64 == b, label_row, 0), axis=1, keepdims=True)
    grid_i = lax.broadcasted_iota(jnp.int32, (64, 64), 0)
    grid_j = lax.broadcasted_iota(jnp.int32, (64, 64), 1)
    label_col = jnp.sum(
        jnp.where(grid_i == grid_j, jnp.broadcast_to(label_row, (64, 64)), 0), axis=1, keepdims=True
    )

    others(NSEQ, s, lambda p: e_copy(s, p).wait_recv())
    embedding = jnp.sum(e_buf[...], axis=0)
    squares = jnp.sum(jnp.sum(embedding * embedding, axis=0, keepdims=True), axis=1, keepdims=True)
    products = jnp.sum(tex[...] * embedding[None], axis=1)
    raw = jnp.sum(products.T, axis=0, keepdims=True)
    logits = raw * lax.rsqrt(squares + 1e-06)
    rows[b] = jnp.concatenate([logits, jnp.zeros((1, 64), F32)], axis=1)
    others(NB1, b_lo, lambda p: b1_copy(p, b_lo).start())

    peak = jnp.max(logits, axis=1, keepdims=True)
    lse = peak + jnp.log(jnp.sum(jnp.exp(logits - peak), axis=1, keepdims=True))
    chosen = jnp.sum(jnp.where(lane64 == own_label, logits, 0.0), axis=1, keepdims=True)
    img_ref[0] = (lse - chosen)[0, 0]
    others(NSEQ, s, lambda p: e_copy(p, s).wait_send())

    others(NB1, b_lo, lambda p: b1_copy(b_lo, p).wait_recv())
    others(NB2, b_hi, lambda p: b2_copy(p, b_hi).start())
    others(NB1, b_lo, lambda p: b1_copy(p, b_lo).wait_send())
    hid_copy.wait()
    others(NB2, b_hi, lambda p: b2_copy(b_hi, p).wait_recv())

    lane128 = lax.broadcasted_iota(jnp.int32, (64, 128), 1)
    column = jnp.sum(jnp.where(lane128 == b, rows[...].reshape(64, 128), 0.0), axis=1, keepdims=True)
    high = jnp.max(column, axis=0, keepdims=True)
    total = high + jnp.log(jnp.sum(jnp.exp(column - high), axis=0, keepdims=True))
    match = jnp.sum(jnp.where(label_col == b, column, 0.0), axis=0, keepdims=True)
    txt_ref[0] = (total - match)[0, 0]
    others(NB2, b_hi, lambda p: b2_copy(p, b_hi).wait_send())


def body(queries, keys, values, residual_in, w_out, ln_gain, w_proj, texts, labels):
    any_space = pl.BlockSpec(memory_space=pl.ANY)
    vmem = pl.BlockSpec(memory_space=pltpu.VMEM)
    smem = pl.BlockSpec(memory_space=pltpu.SMEM)
    dma = pltpu.SemaphoreType.DMA
    out = pl.pallas_call(
        kernel,
        out_shape=(
            jax.ShapeDtypeStruct((1, ROWS, D), BF16),
            jax.ShapeDtypeStruct((1,), F32),
            jax.ShapeDtypeStruct((1,), F32),
        ),
        in_specs=[any_space] * 5 + [vmem, any_space, vmem, vmem],
        out_specs=(any_space, smem, smem),
        scratch_shapes=[
            pltpu.VMEM((ROWS, D), BF16),
            pltpu.VMEM((ROWS, D), BF16),
            pltpu.VMEM((ROWS, D), BF16),
            pltpu.VMEM((ROWS, D), BF16),
            pltpu.VMEM((D, D), BF16),
            pltpu.VMEM((D, EMBED), BF16),
            pltpu.VMEM((ROWS, D), BF16),
            pltpu.VMEM((NSEQ, 2 * HD, ROWS), BF16),
            pltpu.VMEM((NSEQ, HD, ROWS), BF16),
            pltpu.VMEM((NSEQ, 2 * HD, ROWS), BF16),
            pltpu.VMEM((NSEQ, HD, ROWS), BF16),
            pltpu.VMEM((NSEQ, HD, ROWS), BF16),
            pltpu.VMEM((NSEQ, HD, ROWS), BF16),
            pltpu.VMEM((PATCHES, HD), BF16),
            pltpu.VMEM((HD + 16, PATCHES), BF16),
            pltpu.VMEM((PATCHES, CHUNK), F32),
            pltpu.VMEM((ROWS, D), F32),
            pltpu.VMEM((NSEQ, 1, 128), F32),
            pltpu.VMEM((NB, 8, 128), F32),
            pltpu.VMEM((NSEQ, 8, 128), F32),
            pltpu.VMEM((NB, 1, 128), F32),
            dma((8,)),
            dma((NSEQ,)), dma((NSEQ,)),
            dma((NSEQ,)), dma((NSEQ,)),
            dma((NSEQ,)), dma((NSEQ,)),
            dma((NSEQ,)), dma((NSEQ,)),
            dma((NB1,)), dma((NB1,)),
            dma((NB2,)), dma((NB2,)),
            dma((NSEQ,)), dma((NSEQ,)),
            dma((NB1,)), dma((NB1,)),
            dma((NB2,)), dma((NB2,)),
        ],
        compiler_params=pltpu.CompilerParams(
            collective_id=0, has_side_effects=True, vmem_limit_bytes=48 * 1024 * 1024
        ),
        name="attend_and_score",
    )(
        queries.reshape(ROWS, D),
        keys.reshape(ROWS, D),
        values.reshape(ROWS, D),
        residual_in.reshape(ROWS, D),
        w_out,
        ln_gain.reshape(1, D),
        w_proj,
        texts,
        labels.reshape(1, NB),
    )
    return out


def solution(mesh):
    return jax.shard_map(
        body,
        mesh=mesh,
        in_specs=(
            P("batch", "seq", None),
            P("batch", "seq", None),
            P("batch", "seq", None),
            P("batch", "seq", None),
            P(),
            P(),
            P(),
            P("batch", "seq"),
            P(),
        ),
        out_specs=(P("batch", "seq", None), P("batch"), P("batch")),
        check_vma=False,
    )
```

```python
import math

import jax
import jax.numpy as jnp
from jax import lax
from jax.experimental import pallas as pl
from jax.experimental.pallas import tpu as pltpu
from jax.sharding import PartitionSpec as P

HEADS = 16
HD = 80
D = 1280
EMBED = 1024
PATCHES = 2048
ROWS = 128
NSEQ = 16
NZ = 8
NB = 64
NB1 = 16
NB2 = 4
CHUNK = 2 * ROWS
KB = 256
MESH = pl.DeviceIdType.MESH
F32 = jnp.float32
BF16 = jnp.bfloat16


def depth_step(t):
    half = (t + 1) // 2
    return lax.rem(4 + half * (1 - 2 * lax.rem(t, 2)) + NZ, NZ)


def kernel(
    q_hbm, k_hbm, v_hbm, res_hbm, wout_hbm, gain_hbm, wproj_hbm, texts_hbm, labels_hbm,
    hid_hbm, losses_ref,
    q_in, k_in, v_in, res_in, wout, wproj, gain_ref, texts_ref, labels_ref, hid,
    kv_send, q_send, kv_recv, q_recv, o_send, o_recv,
    k_all, vt_all, s_all, acc, t0, tex, e_buf, rows,
    load_sem, kv_ss, kv_rs, q_ss, q_rs, o_ss, o_rs, t0_ss, t0_rs, t1_ss, t1_rs, t2_ss, t2_rs,
    e_ss, e_rs, b1_ss, b1_rs, b2_ss, b2_rs,
):
    b = lax.axis_index("batch")
    s = lax.axis_index("seq")
    z, y = s // 2, lax.rem(s, 2)
    b_hi, b_lo = b // NB1, lax.rem(b, NB1)

    loads = [
        pltpu.make_async_copy(src, dst, load_sem.at[i])
        for i, (src, dst) in enumerate(
            [
                (k_hbm, k_in),
                (v_hbm, v_in),
                (q_hbm, q_in),
                (res_hbm, res_in),
                (wout_hbm, wout),
                (wproj_hbm, wproj),
                (texts_hbm, texts_ref),
                (gain_hbm, gain_ref),
                (labels_hbm, labels_ref),
            ]
        )
    ]
    for i in (0, 1, 6, 2):
        loads[i].start()

    barrier = pltpu.get_barrier_semaphore()

    def greet_seq(r, c):
        pl.semaphore_signal(barrier, inc=1, device_id=(b, lax.rem(s + r, NSEQ)), device_id_type=MESH)
        pl.semaphore_signal(
            barrier, inc=1, device_id=(b_hi * NB1 + lax.rem(b_lo + r, NB1), s), device_id_type=MESH
        )
        return c

    lax.fori_loop(1, NSEQ, greet_seq, 0)

    def greet_far(r, c):
        pl.semaphore_signal(barrier, inc=1, device_id=(lax.rem(b + r * NB1, NB), s), device_id_type=MESH)
        return c

    lax.fori_loop(1, NB2, greet_far, 0)

    def turn(src, put):
        for c in range(D // 128):
            block = src[:, c * 128 : (c + 1) * 128].T
            i = 0
            while i < 8:
                g = c * 8 + i
                n = min(8 - i, 5 - g % 5)
                put(g // 5, (g % 5) * 16, block[i * 16 : (i + n) * 16], n * 16)
                i += n

    def put_k(h, r, value, n):
        kv_send[h, r : r + n, :] = value

    def put_v(h, r, value, n):
        kv_send[h, HD + r : HD + r + n, :] = value

    def put_q(h, r, value, n):
        q_send[h, r : r + n, :] = value

    loads[0].wait()
    turn(k_in, put_k)
    loads[1].wait()
    turn(v_in, put_v)
    for i in (3, 4, 5, 7, 8):
        loads[i].start()

    loads[6].wait()
    piece = texts_ref[...]
    blank = jnp.zeros((1, 64), F32)
    even = jnp.concatenate([piece, blank], axis=1)
    odd = jnp.concatenate([blank, piece], axis=1)
    t0[s] = jnp.where(y == 0, even, odd)

    pl.semaphore_wait(barrier, 2 * (NSEQ - 1) + NB2 - 1)

    def kv_copy(to, frm):
        return pltpu.make_async_remote_copy(
            src_ref=kv_send.at[to], dst_ref=kv_recv.at[frm], send_sem=kv_ss.at[to], recv_sem=kv_rs.at[frm],
            device_id=(b, to), device_id_type=MESH,
        )

    def q_copy(to, frm):
        return pltpu.make_async_remote_copy(
            src_ref=q_send.at[to], dst_ref=q_recv.at[frm], send_sem=q_ss.at[to], recv_sem=q_rs.at[frm],
            device_id=(b, to), device_id_type=MESH,
        )

    def o_copy(to, frm):
        return pltpu.make_async_remote_copy(
            src_ref=o_send.at[to], dst_ref=o_recv.at[frm], send_sem=o_ss.at[to], recv_sem=o_rs.at[frm],
            device_id=(b, to), device_id_type=MESH,
        )

    def t0_copy(to, frm):
        return pltpu.make_async_remote_copy(
            src_ref=t0.at[frm], dst_ref=t0.at[frm], send_sem=t0_ss.at[to], recv_sem=t0_rs.at[frm],
            device_id=(b, to), device_id_type=MESH,
        )

    def e_copy(to, frm):
        return pltpu.make_async_remote_copy(
            src_ref=e_buf.at[frm], dst_ref=e_buf.at[frm], send_sem=e_ss.at[to], recv_sem=e_rs.at[frm],
            device_id=(b, to), device_id_type=MESH,
        )

    def t1_copy(to, frm):
        at = b_hi * NB1 + frm
        return pltpu.make_async_remote_copy(
            src_ref=tex.at[at], dst_ref=tex.at[at], send_sem=t1_ss.at[to], recv_sem=t1_rs.at[frm],
            device_id=(b_hi * NB1 + to, s), device_id_type=MESH,
        )

    def b1_copy(to, frm):
        at = b_hi * NB1 + frm
        return pltpu.make_async_remote_copy(
            src_ref=rows.at[at], dst_ref=rows.at[at], send_sem=b1_ss.at[to], recv_sem=b1_rs.at[frm],
            device_id=(b_hi * NB1 + to, s), device_id_type=MESH,
        )

    def t2_copy(to, frm):
        at = pl.ds(frm * NB1, NB1)
        return pltpu.make_async_remote_copy(
            src_ref=tex.at[at], dst_ref=tex.at[at], send_sem=t2_ss.at[to], recv_sem=t2_rs.at[frm],
            device_id=(to * NB1 + b_lo, s), device_id_type=MESH,
        )

    def b2_copy(to, frm):
        at = pl.ds(frm * NB1, NB1)
        return pltpu.make_async_remote_copy(
            src_ref=rows.at[at], dst_ref=rows.at[at], send_sem=b2_ss.at[to], recv_sem=b2_rs.at[frm],
            device_id=(to * NB1 + b_lo, s), device_id_type=MESH,
        )

    def others(count, me, act):
        def step(r, c):
            act(lax.rem(me + r, count))
            return c

        lax.fori_loop(1, count, step, 0)

    def by_depth(sign, act):
        def step(t, c):
            there = lax.rem(z + sign * depth_step(t) + NZ, NZ)
            for w in range(2):
                peer = 2 * there + lax.rem(y + w, 2)

                @pl.when(peer != s)
                def _():
                    act(peer)

            return c

        lax.fori_loop(0, NZ, step, 0)

    others(NSEQ, s, lambda p: t0_copy(p, s).start())
    by_depth(1, lambda p: kv_copy(p, s).start())

    loads[2].wait()
    turn(q_in, put_q)
    by_depth(1, lambda p: q_copy(p, s).start())

    others(NSEQ, s, lambda p: t0_copy(s, p).wait_recv())
    for k in range(8):
        tex[b, k : k + 1, :] = t0[2 * k] + t0[2 * k + 1]
    others(NB1, b_lo, lambda p: t1_copy(p, b_lo).start())

    kv_recv[s] = kv_send[s]
    q_recv[s] = q_send[s]
    top = lax.broadcasted_iota(jnp.int32, (16, PATCHES), 0)
    vt_all[HD : HD + 16, :] = jnp.where(top == 0, 1.0, 0.0).astype(BF16)

    others(NB1, b_lo, lambda p: t1_copy(b_lo, p).wait_recv())
    others(NB2, b_hi, lambda p: t2_copy(p, b_hi).start())

    def take_kv(t, c):
        there = lax.rem(z - depth_step(t) + NZ, NZ)
        for w in range(2):
            peer = 2 * there + w

            @pl.when(peer != s)
            def _():
                kv_copy(s, peer).wait_recv()

            block = kv_recv[peer]
            k_all[pl.ds(pl.multiple_of((2 * t + w) * ROWS, ROWS), ROWS), :] = block[:HD].T
            vt_all[0:HD, pl.ds(pl.multiple_of((2 * t + w) * ROWS, ROWS), ROWS)] = block[HD:]
        return c

    lax.fori_loop(0, NZ, take_kv, 0)

    loads[3].wait()
    acc[...] = res_in[...].astype(F32)
    factor = HD ** (-0.5) * math.log2(math.e)

    def attend(t, c):
        there = lax.rem(z - depth_step(t) + NZ, NZ)
        for w in range(2):
            peer = 2 * there + w

            @pl.when(peer != s)
            def _():
                q_copy(s, peer).wait_recv()

        qt = jnp.concatenate([q_recv[2 * there], q_recv[2 * there + 1]], axis=1)
        top8 = None
        for i in range(PATCHES // KB):
            part = jnp.dot(k_all[i * KB : (i + 1) * KB, :], qt, preferred_element_type=F32)
            s_all[i * KB : (i + 1) * KB, :] = part
            high = jnp.max(part.reshape(KB // 8, 8, CHUNK), axis=0)
            top8 = high if top8 is None else jnp.maximum(top8, high)
        maxima = jnp.max(top8, axis=0, keepdims=True)
        total = None
        for i in range(PATCHES // KB):
            weights = jnp.exp2((s_all[i * KB : (i + 1) * KB, :] - maxima) * factor).astype(BF16)
            part = jnp.dot(vt_all[:, i * KB : (i + 1) * KB], weights, preferred_element_type=F32)
            total = part if total is None else total + part
        mixed = (total[:HD] / total[HD : HD + 1]).astype(BF16)
        for w in range(2):
            peer = 2 * there + w
            value = mixed[:, w * ROWS : (w + 1) * ROWS]

            @pl.when(peer != s)
            def _():
                o_send[peer] = value
                o_copy(peer, s).start()

            @pl.when(peer == s)
            def _():
                o_recv[s] = value

        return c

    lax.fori_loop(0, NZ, attend, 0)

    others(NSEQ, s, lambda p: kv_copy(p, s).wait_send())
    others(NSEQ, s, lambda p: q_copy(p, s).wait_send())
    others(NSEQ, s, lambda p: t0_copy(p, s).wait_send())
    others(NB1, b_lo, lambda p: t1_copy(p, b_lo).wait_send())
    others(NB2, b_hi, lambda p: t2_copy(p, b_hi).wait_send())
    others(NB2, b_hi, lambda p: t2_copy(b_hi, p).wait_recv())

    loads[4].wait()
    loads[7].wait()
    loads[8].wait()

    def project(t, c):
        there = lax.rem(z + depth_step(t) + NZ, NZ)
        for w in range(2):
            peer = 2 * there + w

            @pl.when(peer != s)
            def _():
                o_copy(s, peer).wait_recv()

        part = jnp.concatenate([o_recv[2 * there], o_recv[2 * there + 1]], axis=0).T
        weight = wout[pl.ds(pl.multiple_of(there * 2 * HD, 2 * HD), 2 * HD), :]
        acc[...] += jnp.dot(part, weight, preferred_element_type=F32)
        return c

    lax.fori_loop(0, NZ, project, 0)

    pool = None
    for i in range(ROWS // 16):
        x = acc[i * 16 : (i + 1) * 16, :]
        hid[i * 16 : (i + 1) * 16, :] = x.astype(BF16)
        centred = x - jnp.sum(x, axis=1, keepdims=True) * (1.0 / D)
        variance = jnp.sum(centred * centred, axis=1, keepdims=True) * (1.0 / D)
        normed = (centred * lax.rsqrt(variance + 1e-05)).reshape(2, 8, D)
        part = normed[0] + normed[1]
        pool = part if pool is None else pool + part
    hid_copy = pltpu.make_async_copy(hid, hid_hbm.at[0], load_sem.at[9])
    hid_copy.start()

    pooled = jnp.sum(pool, axis=0, keepdims=True) * gain_ref[...].reshape(1, D) * (1.0 / PATCHES)
    first = pooled.astype(BF16).astype(F32)
    rest = pooled - first
    second = rest.astype(BF16).astype(F32)
    third = rest - second
    at = lax.broadcasted_iota(jnp.int32, (16, D), 0)
    split = jnp.where(at == 0, first, jnp.where(at == 1, second, jnp.where(at == 2, third, 0.0))).astype(BF16)
    loads[5].wait()
    projected = jnp.sum(jnp.dot(split, wproj[...], preferred_element_type=F32)[0:8], axis=0, keepdims=True)
    for k in range(8):
        e_buf[s, k : k + 1, :] = projected[:, k * 128 : (k + 1) * 128]
    others(NSEQ, s, lambda p: e_copy(p, s).start())

    others(NSEQ, s, lambda p: o_copy(p, s).wait_send())
    label_row = labels_ref[...].reshape(1, NB)
    lane64 = lax.broadcasted_iota(jnp.int32, (1, 64), 1)
    own_label = jnp.sum(jnp.where(lane64 == b, label_row, 0), axis=1, keepdims=True)
    grid_i = lax.broadcasted_iota(jnp.int32, (64, 64), 0)
    grid_j = lax.broadcasted_iota(jnp.int32, (64, 64), 1)
    label_col = jnp.sum(
        jnp.where(grid_i == grid_j, jnp.broadcast_to(label_row, (64, 64)), 0), axis=1, keepdims=True
    )

    others(NSEQ, s, lambda p: e_copy(s, p).wait_recv())
    embedding = jnp.sum(e_buf[...], axis=0)
    squares = jnp.sum(jnp.sum(embedding * embedding, axis=0, keepdims=True), axis=1, keepdims=True)
    products = jnp.sum(tex[...] * embedding[None], axis=1)
    raw = jnp.sum(products.T, axis=0, keepdims=True)
    logits = raw * lax.rsqrt(squares + 1e-06)
    rows[b] = jnp.concatenate([logits, jnp.zeros((1, 64), F32)], axis=1)
    others(NB1, b_lo, lambda p: b1_copy(p, b_lo).start())

    peak = jnp.max(logits, axis=1, keepdims=True)
    lse = peak + jnp.log(jnp.sum(jnp.exp(logits - peak), axis=1, keepdims=True))
    chosen = jnp.sum(jnp.where(lane64 == own_label, logits, 0.0), axis=1, keepdims=True)
    image_loss = lse - chosen
    others(NSEQ, s, lambda p: e_copy(p, s).wait_send())

    others(NB1, b_lo, lambda p: b1_copy(b_lo, p).wait_recv())
    others(NB2, b_hi, lambda p: b2_copy(p, b_hi).start())
    others(NB1, b_lo, lambda p: b1_copy(p, b_lo).wait_send())
    hid_copy.wait()
    others(NB2, b_hi, lambda p: b2_copy(b_hi, p).wait_recv())

    lane128 = lax.broadcasted_iota(jnp.int32, (64, 128), 1)
    column = jnp.sum(jnp.where(lane128 == b, rows[...].reshape(64, 128), 0.0), axis=1, keepdims=True)
    high = jnp.max(column, axis=0, keepdims=True)
    total = high + jnp.log(jnp.sum(jnp.exp(column - high), axis=0, keepdims=True))
    match = jnp.sum(jnp.where(label_col == b, column, 0.0), axis=0, keepdims=True)
    losses_ref[...] = jnp.where(lax.broadcasted_iota(jnp.int32, (1, 128), 1) == 0, image_loss, total - match)
    others(NB2, b_hi, lambda p: b2_copy(p, b_hi).wait_send())


def body(queries, keys, values, residual_in, w_out, ln_gain, w_proj, texts, labels):
    any_space = pl.BlockSpec(memory_space=pltpu.HBM)
    dma = pltpu.SemaphoreType.DMA
    hidden_out, losses = pl.pallas_call(
        kernel,
        out_shape=(
            jax.ShapeDtypeStruct((1, ROWS, D), BF16),
            jax.ShapeDtypeStruct((1, 128), F32),
        ),
        in_specs=[any_space] * 9,
        out_specs=(any_space, pl.BlockSpec(memory_space=pltpu.VMEM)),
        scratch_shapes=[
            pltpu.VMEM((ROWS, D), BF16),
            pltpu.VMEM((ROWS, D), BF16),
            pltpu.VMEM((ROWS, D), BF16),
            pltpu.VMEM((ROWS, D), BF16),
            pltpu.VMEM((D, D), BF16),
            pltpu.VMEM((D, EMBED), BF16),
            pltpu.VMEM((D,), F32),
            pltpu.VMEM((1, 64), F32),
            pltpu.VMEM((NB,), jnp.int32),
            pltpu.VMEM((ROWS, D), BF16),
            pltpu.VMEM((NSEQ, 2 * HD, ROWS), BF16),
            pltpu.VMEM((NSEQ, HD, ROWS), BF16),
            pltpu.VMEM((NSEQ, 2 * HD, ROWS), BF16),
            pltpu.VMEM((NSEQ, HD, ROWS), BF16),
            pltpu.VMEM((NSEQ, HD, ROWS), BF16),
            pltpu.VMEM((NSEQ, HD, ROWS), BF16),
            pltpu.VMEM((PATCHES, HD), BF16),
            pltpu.VMEM((HD + 16, PATCHES), BF16),
            pltpu.VMEM((PATCHES, CHUNK), F32),
            pltpu.VMEM((ROWS, D), F32),
            pltpu.VMEM((NSEQ, 1, 128), F32),
            pltpu.VMEM((NB, 8, 128), F32),
            pltpu.VMEM((NSEQ, 8, 128), F32),
            pltpu.VMEM((NB, 1, 128), F32),
            dma((10,)),
            dma((NSEQ,)), dma((NSEQ,)),
            dma((NSEQ,)), dma((NSEQ,)),
            dma((NSEQ,)), dma((NSEQ,)),
            dma((NSEQ,)), dma((NSEQ,)),
            dma((NB1,)), dma((NB1,)),
            dma((NB2,)), dma((NB2,)),
            dma((NSEQ,)), dma((NSEQ,)),
            dma((NB1,)), dma((NB1,)),
            dma((NB2,)), dma((NB2,)),
        ],
        compiler_params=pltpu.CompilerParams(
            collective_id=0, has_side_effects=True, vmem_limit_bytes=67043328
        ),
        name="attend_and_score",
    )(
        queries.reshape(ROWS, D),
        keys.reshape(ROWS, D),
        values.reshape(ROWS, D),
        residual_in.reshape(ROWS, D),
        w_out,
        ln_gain,
        w_proj,
        texts,
        labels,
    )
    return hidden_out, losses[0, 0:1], losses[0, 1:2]


def solution(mesh):
    return jax.shard_map(
        body,
        mesh=mesh,
        in_specs=(
            P("batch", "seq", None),
            P("batch", "seq", None),
            P("batch", "seq", None),
            P("batch", "seq", None),
            P(),
            P(),
            P(),
            P("batch", "seq"),
            P(),
        ),
        out_specs=(P("batch", "seq", None), P("batch"), P("batch")),
        check_vma=False,
    )
```

```python
import math

import jax
import jax.numpy as jnp
from jax import lax
from jax.experimental import pallas as pl
from jax.experimental.pallas import tpu as pltpu
from jax.sharding import PartitionSpec as P

HEADS = 16
HD = 80
D = 1280
EMBED = 1024
PATCHES = 2048
ROWS = 128
NSEQ = 16
NZ = 8
NB = 64
NB1 = 16
NB2 = 4
CHUNK = 2 * ROWS
KB = 256
MESH = pl.DeviceIdType.MESH
F32 = jnp.float32
BF16 = jnp.bfloat16


def depth_step(t):
    half = (t + 1) // 2
    return lax.rem(4 + half * (1 - 2 * lax.rem(t, 2)) + NZ, NZ)


def kernel(
    q_hbm, k_hbm, v_hbm, res_hbm, wout_hbm, gain_hbm, wproj_hbm, texts_hbm, labels_hbm,
    hid_hbm, losses_hbm,
    q_in, k_in, v_in, res_in, wout, wproj, gain_ref, texts_ref, labels_ref, hid, losses_ref,
    kv_send, q_send, kv_recv, q_recv, o_send, o_recv,
    k_all, vt_all, s_all, acc, t0, tex, e_buf, rows,
    load_sem, kv_ss, kv_rs, q_ss, q_rs, o_ss, o_rs, t0_ss, t0_rs, t1_ss, t1_rs, t2_ss, t2_rs,
    e_ss, e_rs, b1_ss, b1_rs, b2_ss, b2_rs,
):
    b = lax.axis_index("batch")
    s = lax.axis_index("seq")
    z, y = s // 2, lax.rem(s, 2)
    b_hi, b_lo = b // NB1, lax.rem(b, NB1)

    loads = [
        pltpu.make_async_copy(src, dst, load_sem.at[i])
        for i, (src, dst) in enumerate(
            [
                (k_hbm, k_in),
                (v_hbm, v_in),
                (q_hbm, q_in),
                (res_hbm, res_in),
                (wout_hbm, wout),
                (wproj_hbm, wproj),
                (texts_hbm, texts_ref),
                (gain_hbm, gain_ref),
                (labels_hbm, labels_ref),
            ]
        )
    ]
    for i in (0, 1, 6, 2):
        loads[i].start()

    barrier = pltpu.get_barrier_semaphore()

    def greet_seq(r, c):
        pl.semaphore_signal(barrier, inc=1, device_id=(b, lax.rem(s + r, NSEQ)), device_id_type=MESH)
        pl.semaphore_signal(
            barrier, inc=1, device_id=(b_hi * NB1 + lax.rem(b_lo + r, NB1), s), device_id_type=MESH
        )
        return c

    lax.fori_loop(1, NSEQ, greet_seq, 0)

    def greet_far(r, c):
        pl.semaphore_signal(barrier, inc=1, device_id=(lax.rem(b + r * NB1, NB), s), device_id_type=MESH)
        return c

    lax.fori_loop(1, NB2, greet_far, 0)

    def turn(src, put):
        for c in range(D // 128):
            block = src[:, c * 128 : (c + 1) * 128].T
            i = 0
            while i < 8:
                g = c * 8 + i
                n = min(8 - i, 5 - g % 5)
                put(g // 5, (g % 5) * 16, block[i * 16 : (i + n) * 16], n * 16)
                i += n

    def put_k(h, r, value, n):
        kv_send[h, r : r + n, :] = value

    def put_v(h, r, value, n):
        kv_send[h, HD + r : HD + r + n, :] = value

    def put_q(h, r, value, n):
        q_send[h, r : r + n, :] = value

    loads[0].wait()
    turn(k_in, put_k)
    loads[1].wait()
    turn(v_in, put_v)
    for i in (3, 4, 5, 7, 8):
        loads[i].start()

    loads[6].wait()
    piece = texts_ref[...]
    blank = jnp.zeros((1, 64), F32)
    even = jnp.concatenate([piece, blank], axis=1)
    odd = jnp.concatenate([blank, piece], axis=1)
    t0[s] = jnp.where(y == 0, even, odd)

    pl.semaphore_wait(barrier, 2 * (NSEQ - 1) + NB2 - 1)

    def kv_copy(to, frm):
        return pltpu.make_async_remote_copy(
            src_ref=kv_send.at[to], dst_ref=kv_recv.at[frm], send_sem=kv_ss.at[to], recv_sem=kv_rs.at[frm],
            device_id=(b, to), device_id_type=MESH,
        )

    def q_copy(to, frm):
        return pltpu.make_async_remote_copy(
            src_ref=q_send.at[to], dst_ref=q_recv.at[frm], send_sem=q_ss.at[to], recv_sem=q_rs.at[frm],
            device_id=(b, to), device_id_type=MESH,
        )

    def o_copy(to, frm):
        return pltpu.make_async_remote_copy(
            src_ref=o_send.at[to], dst_ref=o_recv.at[frm], send_sem=o_ss.at[to], recv_sem=o_rs.at[frm],
            device_id=(b, to), device_id_type=MESH,
        )

    def t0_copy(to, frm):
        return pltpu.make_async_remote_copy(
            src_ref=t0.at[frm], dst_ref=t0.at[frm], send_sem=t0_ss.at[to], recv_sem=t0_rs.at[frm],
            device_id=(b, to), device_id_type=MESH,
        )

    def e_copy(to, frm):
        return pltpu.make_async_remote_copy(
            src_ref=e_buf.at[frm], dst_ref=e_buf.at[frm], send_sem=e_ss.at[to], recv_sem=e_rs.at[frm],
            device_id=(b, to), device_id_type=MESH,
        )

    def t1_copy(to, frm):
        at = b_hi * NB1 + frm
        return pltpu.make_async_remote_copy(
            src_ref=tex.at[at], dst_ref=tex.at[at], send_sem=t1_ss.at[to], recv_sem=t1_rs.at[frm],
            device_id=(b_hi * NB1 + to, s), device_id_type=MESH,
        )

    def b1_copy(to, frm):
        at = b_hi * NB1 + frm
        return pltpu.make_async_remote_copy(
            src_ref=rows.at[at], dst_ref=rows.at[at], send_sem=b1_ss.at[to], recv_sem=b1_rs.at[frm],
            device_id=(b_hi * NB1 + to, s), device_id_type=MESH,
        )

    def t2_copy(to, frm):
        at = pl.ds(frm * NB1, NB1)
        return pltpu.make_async_remote_copy(
            src_ref=tex.at[at], dst_ref=tex.at[at], send_sem=t2_ss.at[to], recv_sem=t2_rs.at[frm],
            device_id=(to * NB1 + b_lo, s), device_id_type=MESH,
        )

    def b2_copy(to, frm):
        at = pl.ds(frm * NB1, NB1)
        return pltpu.make_async_remote_copy(
            src_ref=rows.at[at], dst_ref=rows.at[at], send_sem=b2_ss.at[to], recv_sem=b2_rs.at[frm],
            device_id=(to * NB1 + b_lo, s), device_id_type=MESH,
        )

    def others(count, me, act):
        def step(r, c):
            act(lax.rem(me + r, count))
            return c

        lax.fori_loop(1, count, step, 0)

    def by_depth(sign, act):
        def step(t, c):
            there = lax.rem(z + sign * depth_step(t) + NZ, NZ)
            for w in range(2):
                peer = 2 * there + lax.rem(y + w, 2)

                @pl.when(peer != s)
                def _():
                    act(peer)

            return c

        lax.fori_loop(0, NZ, step, 0)

    others(NSEQ, s, lambda p: t0_copy(p, s).start())
    by_depth(1, lambda p: kv_copy(p, s).start())

    loads[2].wait()
    turn(q_in, put_q)
    by_depth(1, lambda p: q_copy(p, s).start())

    kv_recv[s] = kv_send[s]
    q_recv[s] = q_send[s]
    top = lax.broadcasted_iota(jnp.int32, (16, PATCHES), 0)
    vt_all[HD : HD + 16, :] = jnp.where(top == 0, 1.0, 0.0).astype(BF16)

    def take_kv(t, c):
        there = lax.rem(z - depth_step(t) + NZ, NZ)
        for w in range(2):
            peer = 2 * there + w

            @pl.when(peer != s)
            def _():
                kv_copy(s, peer).wait_recv()

            block = kv_recv[peer]
            k_all[pl.ds(pl.multiple_of((2 * t + w) * ROWS, ROWS), ROWS), :] = block[:HD].T
            vt_all[0:HD, pl.ds(pl.multiple_of((2 * t + w) * ROWS, ROWS), ROWS)] = block[HD:]
        return c

    lax.fori_loop(0, NZ, take_kv, 0)

    others(NSEQ, s, lambda p: t0_copy(s, p).wait_recv())
    for k in range(8):
        tex[b, k : k + 1, :] = t0[2 * k] + t0[2 * k + 1]
    others(NB1, b_lo, lambda p: t1_copy(p, b_lo).start())

    loads[3].wait()
    acc[...] = res_in[...].astype(F32)
    factor = HD ** (-0.5) * math.log2(math.e)

    def attend(t, c):
        there = lax.rem(z - depth_step(t) + NZ, NZ)
        for w in range(2):
            peer = 2 * there + w

            @pl.when(peer != s)
            def _():
                q_copy(s, peer).wait_recv()

        qt = jnp.concatenate([q_recv[2 * there], q_recv[2 * there + 1]], axis=1)
        top8 = None
        for i in range(PATCHES // KB):
            part = jnp.dot(k_all[i * KB : (i + 1) * KB, :], qt, preferred_element_type=F32)
            s_all[i * KB : (i + 1) * KB, :] = part
            high = jnp.max(part.reshape(KB // 8, 8, CHUNK), axis=0)
            top8 = high if top8 is None else jnp.maximum(top8, high)
        maxima = jnp.max(top8, axis=0, keepdims=True)
        total = None
        for i in range(PATCHES // KB):
            weights = jnp.exp2((s_all[i * KB : (i + 1) * KB, :] - maxima) * factor).astype(BF16)
            part = jnp.dot(vt_all[:, i * KB : (i + 1) * KB], weights, preferred_element_type=F32)
            total = part if total is None else total + part
        mixed = (total[:HD] / total[HD : HD + 1]).astype(BF16)
        for w in range(2):
            peer = 2 * there + w
            value = mixed[:, w * ROWS : (w + 1) * ROWS]

            @pl.when(peer != s)
            def _():
                o_send[peer] = value
                o_copy(peer, s).start()

            @pl.when(peer == s)
            def _():
                o_recv[s] = value

        return c

    lax.fori_loop(0, NZ, attend, 0)

    others(NB1, b_lo, lambda p: t1_copy(b_lo, p).wait_recv())
    others(NB2, b_hi, lambda p: t2_copy(p, b_hi).start())
    others(NSEQ, s, lambda p: kv_copy(p, s).wait_send())
    others(NSEQ, s, lambda p: q_copy(p, s).wait_send())
    others(NSEQ, s, lambda p: t0_copy(p, s).wait_send())
    others(NB1, b_lo, lambda p: t1_copy(p, b_lo).wait_send())

    loads[4].wait()
    loads[7].wait()
    loads[8].wait()

    def project(t, c):
        there = lax.rem(z + depth_step(t) + NZ, NZ)
        for w in range(2):
            peer = 2 * there + w

            @pl.when(peer != s)
            def _():
                o_copy(s, peer).wait_recv()

        part = jnp.concatenate([o_recv[2 * there], o_recv[2 * there + 1]], axis=0).T
        weight = wout[pl.ds(pl.multiple_of(there * 2 * HD, 2 * HD), 2 * HD), :]
        acc[...] += jnp.dot(part, weight, preferred_element_type=F32)
        return c

    lax.fori_loop(0, NZ, project, 0)

    pool = None
    for i in range(ROWS // 16):
        x = acc[i * 16 : (i + 1) * 16, :]
        hid[i * 16 : (i + 1) * 16, :] = x.astype(BF16)
        centred = x - jnp.sum(x, axis=1, keepdims=True) * (1.0 / D)
        variance = jnp.sum(centred * centred, axis=1, keepdims=True) * (1.0 / D)
        normed = (centred * lax.rsqrt(variance + 1e-05)).reshape(2, 8, D)
        part = normed[0] + normed[1]
        pool = part if pool is None else pool + part
    hid_copy = pltpu.make_async_copy(hid, hid_hbm.at[0], load_sem.at[9])
    hid_copy.start()

    pooled = jnp.sum(pool, axis=0, keepdims=True) * gain_ref[...].reshape(1, D) * (1.0 / PATCHES)
    first = pooled.astype(BF16).astype(F32)
    rest = pooled - first
    second = rest.astype(BF16).astype(F32)
    third = rest - second
    at = lax.broadcasted_iota(jnp.int32, (16, D), 0)
    split = jnp.where(at == 0, first, jnp.where(at == 1, second, jnp.where(at == 2, third, 0.0))).astype(BF16)
    loads[5].wait()
    projected = jnp.sum(jnp.dot(split, wproj[...], preferred_element_type=F32)[0:8], axis=0, keepdims=True)
    for k in range(8):
        e_buf[s, k : k + 1, :] = projected[:, k * 128 : (k + 1) * 128]
    others(NSEQ, s, lambda p: e_copy(p, s).start())

    others(NSEQ, s, lambda p: o_copy(p, s).wait_send())
    label_row = labels_ref[...].reshape(1, NB)
    lane64 = lax.broadcasted_iota(jnp.int32, (1, 64), 1)
    own_label = jnp.sum(jnp.where(lane64 == b, label_row, 0), axis=1, keepdims=True)
    grid_i = lax.broadcasted_iota(jnp.int32, (64, 64), 0)
    grid_j = lax.broadcasted_iota(jnp.int32, (64, 64), 1)
    label_col = jnp.sum(
        jnp.where(grid_i == grid_j, jnp.broadcast_to(label_row, (64, 64)), 0), axis=1, keepdims=True
    )

    others(NB2, b_hi, lambda p: t2_copy(p, b_hi).wait_send())
    others(NB2, b_hi, lambda p: t2_copy(b_hi, p).wait_recv())
    others(NSEQ, s, lambda p: e_copy(s, p).wait_recv())
    embedding = jnp.sum(e_buf[...], axis=0)
    squares = jnp.sum(jnp.sum(embedding * embedding, axis=0, keepdims=True), axis=1, keepdims=True)
    products = jnp.sum(tex[...] * embedding[None], axis=1)
    raw = jnp.sum(products.T, axis=0, keepdims=True)
    logits = raw * lax.rsqrt(squares + 1e-06)
    rows[b] = jnp.concatenate([logits, jnp.zeros((1, 64), F32)], axis=1)
    others(NB1, b_lo, lambda p: b1_copy(p, b_lo).start())

    peak = jnp.max(logits, axis=1, keepdims=True)
    lse = peak + jnp.log(jnp.sum(jnp.exp(logits - peak), axis=1, keepdims=True))
    chosen = jnp.sum(jnp.where(lane64 == own_label, logits, 0.0), axis=1, keepdims=True)
    image_loss = lse - chosen
    others(NSEQ, s, lambda p: e_copy(p, s).wait_send())

    others(NB1, b_lo, lambda p: b1_copy(b_lo, p).wait_recv())
    others(NB2, b_hi, lambda p: b2_copy(p, b_hi).start())
    others(NB1, b_lo, lambda p: b1_copy(p, b_lo).wait_send())
    hid_copy.wait()
    others(NB2, b_hi, lambda p: b2_copy(b_hi, p).wait_recv())

    lane128 = lax.broadcasted_iota(jnp.int32, (64, 128), 1)
    column = jnp.sum(jnp.where(lane128 == b, rows[...].reshape(64, 128), 0.0), axis=1, keepdims=True)
    high = jnp.max(column, axis=0, keepdims=True)
    total = high + jnp.log(jnp.sum(jnp.exp(column - high), axis=0, keepdims=True))
    match = jnp.sum(jnp.where(label_col == b, column, 0.0), axis=0, keepdims=True)
    losses_ref[...] = jnp.where(lax.broadcasted_iota(jnp.int32, (1, 128), 1) == 0, image_loss, total - match)
    losses_copy = pltpu.make_async_copy(losses_ref, losses_hbm, load_sem.at[0])
    losses_copy.start()
    others(NB2, b_hi, lambda p: b2_copy(p, b_hi).wait_send())
    losses_copy.wait()


def body(queries, keys, values, residual_in, w_out, ln_gain, w_proj, texts, labels):
    far_space = pl.BlockSpec(memory_space=pltpu.HBM)
    any_space = pl.BlockSpec(memory_space=pl.ANY)
    dma = pltpu.SemaphoreType.DMA
    hidden_out, losses = pl.pallas_call(
        kernel,
        out_shape=(
            jax.ShapeDtypeStruct((1, ROWS, D), BF16),
            jax.ShapeDtypeStruct((1, 128), F32),
        ),
        in_specs=[far_space] * 9,
        out_specs=(any_space, any_space),
        scratch_shapes=[
            pltpu.VMEM((ROWS, D), BF16),
            pltpu.VMEM((ROWS, D), BF16),
            pltpu.VMEM((ROWS, D), BF16),
            pltpu.VMEM((ROWS, D), BF16),
            pltpu.VMEM((D, D), BF16),
            pltpu.VMEM((D, EMBED), BF16),
            pltpu.VMEM((D,), F32),
            pltpu.VMEM((1, 64), F32),
            pltpu.VMEM((NB,), jnp.int32),
            pltpu.VMEM((ROWS, D), BF16),
            pltpu.VMEM((1, 128), F32),
            pltpu.VMEM((NSEQ, 2 * HD, ROWS), BF16),
            pltpu.VMEM((NSEQ, HD, ROWS), BF16),
            pltpu.VMEM((NSEQ, 2 * HD, ROWS), BF16),
            pltpu.VMEM((NSEQ, HD, ROWS), BF16),
            pltpu.VMEM((NSEQ, HD, ROWS), BF16),
            pltpu.VMEM((NSEQ, HD, ROWS), BF16),
            pltpu.VMEM((PATCHES, HD), BF16),
            pltpu.VMEM((HD + 16, PATCHES), BF16),
            pltpu.VMEM((PATCHES, CHUNK), F32),
            pltpu.VMEM((ROWS, D), F32),
            pltpu.VMEM((NSEQ, 1, 128), F32),
            pltpu.VMEM((NB, 8, 128), F32),
            pltpu.VMEM((NSEQ, 8, 128), F32),
            pltpu.VMEM((NB, 1, 128), F32),
            dma((10,)),
            dma((NSEQ,)), dma((NSEQ,)),
            dma((NSEQ,)), dma((NSEQ,)),
            dma((NSEQ,)), dma((NSEQ,)),
            dma((NSEQ,)), dma((NSEQ,)),
            dma((NB1,)), dma((NB1,)),
            dma((NB2,)), dma((NB2,)),
            dma((NSEQ,)), dma((NSEQ,)),
            dma((NB1,)), dma((NB1,)),
            dma((NB2,)), dma((NB2,)),
        ],
        compiler_params=pltpu.CompilerParams(
            collective_id=0, has_side_effects=True, vmem_limit_bytes=67043328
        ),
        name="attend_and_score",
    )(
        queries.reshape(ROWS, D),
        keys.reshape(ROWS, D),
        values.reshape(ROWS, D),
        residual_in.reshape(ROWS, D),
        w_out,
        ln_gain,
        w_proj,
        texts,
        labels,
    )
    return hidden_out, losses[0, 0:1], losses[0, 1:2]


def solution(mesh):
    return jax.shard_map(
        body,
        mesh=mesh,
        in_specs=(
            P("batch", "seq", None),
            P("batch", "seq", None),
            P("batch", "seq", None),
            P("batch", "seq", None),
            P(),
            P(),
            P(),
            P("batch", "seq"),
            P(),
        ),
        out_specs=(P("batch", "seq", None), P("batch"), P("batch")),
        check_vma=False,
    )
```

```python
import math

import jax
import jax.numpy as jnp
from jax import lax
from jax.experimental import pallas as pl
from jax.experimental.pallas import tpu as pltpu
from jax.sharding import PartitionSpec as P

HEADS = 16
HD = 80
D = 1280
EMBED = 1024
PATCHES = 2048
ROWS = 128
NSEQ = 16
NZ = 8
NB = 64
NB1 = 16
NB2 = 4
CHUNK = 2 * ROWS
KB = 256
MESH = pl.DeviceIdType.MESH
F32 = jnp.float32
BF16 = jnp.bfloat16


def depth_step(t):
    half = (t + 1) // 2
    return lax.rem(4 + half * (1 - 2 * lax.rem(t, 2)) + NZ, NZ)


def kernel(
    q_hbm, k_hbm, v_hbm, res_hbm, wout_hbm, gain_hbm, wproj_hbm, texts_hbm, labels_hbm,
    hid_hbm, losses_hbm,
    q_in, k_in, v_in, res_in, wout, wproj, gain_ref, texts_ref, labels_ref, hid, losses_ref,
    kv_send, q_send, kv_recv, q_recv, o_send, o_recv,
    k_all, vt_all, s_all, acc, t0, tex, e_buf, rows,
    load_sem, kv_ss, kv_rs, q_ss, q_rs, o_ss, o_rs, t0_ss, t0_rs, t1_ss, t1_rs, t2_ss, t2_rs,
    e_ss, e_rs, b1_ss, b1_rs, b2_ss, b2_rs,
):
    b = lax.axis_index("batch")
    s = lax.axis_index("seq")
    z, y = s // 2, lax.rem(s, 2)
    b_hi, b_lo = b // NB1, lax.rem(b, NB1)

    loads = [
        pltpu.make_async_copy(src, dst, load_sem.at[i])
        for i, (src, dst) in enumerate(
            [
                (k_hbm, k_in),
                (v_hbm, v_in),
                (q_hbm, q_in),
                (res_hbm, res_in),
                (wout_hbm, wout),
                (wproj_hbm, wproj),
                (texts_hbm, texts_ref),
                (gain_hbm, gain_ref),
                (labels_hbm, labels_ref),
            ]
        )
    ]
    for i in (0, 1, 6, 2):
        loads[i].start()

    barrier = pltpu.get_barrier_semaphore()

    def greet_seq(r, c):
        pl.semaphore_signal(barrier, inc=1, device_id=(b, lax.rem(s + r, NSEQ)), device_id_type=MESH)
        pl.semaphore_signal(
            barrier, inc=1, device_id=(b_hi * NB1 + lax.rem(b_lo + r, NB1), s), device_id_type=MESH
        )
        return c

    lax.fori_loop(1, NSEQ, greet_seq, 0)

    def greet_far(r, c):
        pl.semaphore_signal(barrier, inc=1, device_id=(lax.rem(b + r * NB1, NB), s), device_id_type=MESH)
        return c

    lax.fori_loop(1, NB2, greet_far, 0)

    def turn(src, put):
        for c in range(D // 128):
            block = src[:, c * 128 : (c + 1) * 128].T
            i = 0
            while i < 8:
                g = c * 8 + i
                n = min(8 - i, 5 - g % 5)
                put(g // 5, (g % 5) * 16, block[i * 16 : (i + n) * 16], n * 16)
                i += n

    def put_k(h, r, value, n):
        kv_send[h, r : r + n, :] = value

    def put_v(h, r, value, n):
        kv_send[h, HD + r : HD + r + n, :] = value

    def put_q(h, r, value, n):
        q_send[h, r : r + n, :] = value

    loads[0].wait()
    turn(k_in, put_k)
    loads[1].wait()
    turn(v_in, put_v)
    for i in (3, 4, 5, 7, 8):
        loads[i].start()

    loads[6].wait()
    piece = texts_ref[...]
    blank = jnp.zeros((1, 64), F32)
    even = jnp.concatenate([piece, blank], axis=1)
    odd = jnp.concatenate([blank, piece], axis=1)
    t0[s] = jnp.where(y == 0, even, odd)

    pl.semaphore_wait(barrier, 2 * (NSEQ - 1) + NB2 - 1)

    def kv_copy(to, frm):
        return pltpu.make_async_remote_copy(
            src_ref=kv_send.at[to], dst_ref=kv_recv.at[frm], send_sem=kv_ss.at[0], recv_sem=kv_rs.at[frm],
            device_id=(b, to), device_id_type=MESH,
        )

    def q_copy(to, frm):
        return pltpu.make_async_remote_copy(
            src_ref=q_send.at[to], dst_ref=q_recv.at[frm], send_sem=q_ss.at[0], recv_sem=q_rs.at[frm],
            device_id=(b, to), device_id_type=MESH,
        )

    def o_copy(to, frm):
        return pltpu.make_async_remote_copy(
            src_ref=o_send.at[to], dst_ref=o_recv.at[frm], send_sem=o_ss.at[0], recv_sem=o_rs.at[frm],
            device_id=(b, to), device_id_type=MESH,
        )

    def t0_copy(to, frm):
        return pltpu.make_async_remote_copy(
            src_ref=t0.at[frm], dst_ref=t0.at[frm], send_sem=t0_ss.at[0], recv_sem=t0_rs.at[0],
            device_id=(b, to), device_id_type=MESH,
        )

    def e_copy(to, frm):
        return pltpu.make_async_remote_copy(
            src_ref=e_buf.at[frm], dst_ref=e_buf.at[frm], send_sem=e_ss.at[0], recv_sem=e_rs.at[0],
            device_id=(b, to), device_id_type=MESH,
        )

    def t1_copy(to, frm):
        at = b_hi * NB1 + frm
        return pltpu.make_async_remote_copy(
            src_ref=tex.at[at], dst_ref=tex.at[at], send_sem=t1_ss.at[0], recv_sem=t1_rs.at[0],
            device_id=(b_hi * NB1 + to, s), device_id_type=MESH,
        )

    def b1_copy(to, frm):
        at = b_hi * NB1 + frm
        return pltpu.make_async_remote_copy(
            src_ref=rows.at[at], dst_ref=rows.at[at], send_sem=b1_ss.at[0], recv_sem=b1_rs.at[0],
            device_id=(b_hi * NB1 + to, s), device_id_type=MESH,
        )

    def t2_copy(to, frm):
        at = pl.ds(frm * NB1, NB1)
        return pltpu.make_async_remote_copy(
            src_ref=tex.at[at], dst_ref=tex.at[at], send_sem=t2_ss.at[0], recv_sem=t2_rs.at[0],
            device_id=(to * NB1 + b_lo, s), device_id_type=MESH,
        )

    def b2_copy(to, frm):
        at = pl.ds(frm * NB1, NB1)
        return pltpu.make_async_remote_copy(
            src_ref=rows.at[at], dst_ref=rows.at[at], send_sem=b2_ss.at[0], recv_sem=b2_rs.at[0],
            device_id=(to * NB1 + b_lo, s), device_id_type=MESH,
        )

    def whole(ref, count, send_sem, recv_sem):
        part = ref.at[pl.ds(0, count)]
        return pltpu.make_async_remote_copy(
            src_ref=part, dst_ref=part, send_sem=send_sem.at[0], recv_sem=recv_sem.at[0],
            device_id=(b, lax.rem(s + 1, NSEQ)), device_id_type=MESH,
        )

    def others(count, me, act):
        def step(r, c):
            act(lax.rem(me + r, count))
            return c

        lax.fori_loop(1, count, step, 0)

    def by_depth(sign, act):
        def step(t, c):
            there = lax.rem(z + sign * depth_step(t) + NZ, NZ)
            for w in range(2):
                peer = 2 * there + lax.rem(y + w, 2)

                @pl.when(peer != s)
                def _():
                    act(peer)

            return c

        lax.fori_loop(0, NZ, step, 0)

    others(NSEQ, s, lambda p: t0_copy(p, s).start())
    by_depth(1, lambda p: kv_copy(p, s).start())

    loads[2].wait()
    turn(q_in, put_q)
    by_depth(1, lambda p: q_copy(p, s).start())

    kv_recv[s] = kv_send[s]
    q_recv[s] = q_send[s]
    top = lax.broadcasted_iota(jnp.int32, (16, PATCHES), 0)
    vt_all[HD : HD + 16, :] = jnp.where(top == 0, 1.0, 0.0).astype(BF16)

    def take_kv(t, c):
        there = lax.rem(z - depth_step(t) + NZ, NZ)
        for w in range(2):
            peer = 2 * there + w

            @pl.when(peer != s)
            def _():
                kv_copy(s, peer).wait_recv()

            block = kv_recv[peer]
            k_all[pl.ds(pl.multiple_of((2 * t + w) * ROWS, ROWS), ROWS), :] = block[:HD].T
            vt_all[0:HD, pl.ds(pl.multiple_of((2 * t + w) * ROWS, ROWS), ROWS)] = block[HD:]
        return c

    lax.fori_loop(0, NZ, take_kv, 0)

    whole(t0, NSEQ - 1, t0_ss, t0_rs).wait_recv()
    for k in range(8):
        tex[b, k : k + 1, :] = t0[2 * k] + t0[2 * k + 1]
    others(NB1, b_lo, lambda p: t1_copy(p, b_lo).start())

    loads[3].wait()
    acc[...] = res_in[...].astype(F32)
    factor = HD ** (-0.5) * math.log2(math.e)

    def attend(t, c):
        @pl.when(t == 4)
        def _():
            whole(tex, NB1 - 1, t1_ss, t1_rs).wait_recv()
            others(NB2, b_hi, lambda p: t2_copy(p, b_hi).start())

        there = lax.rem(z - depth_step(t) + NZ, NZ)
        for w in range(2):
            peer = 2 * there + w

            @pl.when(peer != s)
            def _():
                q_copy(s, peer).wait_recv()

        qt = jnp.concatenate([q_recv[2 * there], q_recv[2 * there + 1]], axis=1)
        top8 = None
        for i in range(PATCHES // KB):
            part = jnp.dot(k_all[i * KB : (i + 1) * KB, :], qt, preferred_element_type=F32)
            s_all[i * KB : (i + 1) * KB, :] = part
            high = jnp.max(part.reshape(KB // 8, 8, CHUNK), axis=0)
            top8 = high if top8 is None else jnp.maximum(top8, high)
        maxima = jnp.max(top8, axis=0, keepdims=True)
        total = None
        for i in range(PATCHES // KB):
            weights = jnp.exp2((s_all[i * KB : (i + 1) * KB, :] - maxima) * factor).astype(BF16)
            part = jnp.dot(vt_all[:, i * KB : (i + 1) * KB], weights, preferred_element_type=F32)
            total = part if total is None else total + part
        mixed = (total[:HD] / total[HD : HD + 1]).astype(BF16)
        for w in range(2):
            peer = 2 * there + w
            value = mixed[:, w * ROWS : (w + 1) * ROWS]

            @pl.when(peer != s)
            def _():
                o_send[peer] = value
                o_copy(peer, s).start()

            @pl.when(peer == s)
            def _():
                o_recv[s] = value

        return c

    lax.fori_loop(0, NZ, attend, 0)

    whole(kv_send, NSEQ - 1, kv_ss, kv_rs).wait_send()
    whole(q_send, NSEQ - 1, q_ss, q_rs).wait_send()
    whole(t0, NSEQ - 1, t0_ss, t0_rs).wait_send()
    whole(tex, NB1 - 1, t1_ss, t1_rs).wait_send()

    loads[4].wait()
    loads[7].wait()
    loads[8].wait()

    def project(t, c):
        there = lax.rem(z + depth_step(t) + NZ, NZ)
        for w in range(2):
            peer = 2 * there + w

            @pl.when(peer != s)
            def _():
                o_copy(s, peer).wait_recv()

        part = jnp.concatenate([o_recv[2 * there], o_recv[2 * there + 1]], axis=0).T
        weight = wout[pl.ds(pl.multiple_of(there * 2 * HD, 2 * HD), 2 * HD), :]
        acc[...] += jnp.dot(part, weight, preferred_element_type=F32)
        return c

    lax.fori_loop(0, NZ, project, 0)

    pool = None
    for i in range(ROWS // 16):
        x = acc[i * 16 : (i + 1) * 16, :]
        hid[i * 16 : (i + 1) * 16, :] = x.astype(BF16)
        centred = x - jnp.sum(x, axis=1, keepdims=True) * (1.0 / D)
        variance = jnp.sum(centred * centred, axis=1, keepdims=True) * (1.0 / D)
        normed = (centred * lax.rsqrt(variance + 1e-05)).reshape(2, 8, D)
        part = normed[0] + normed[1]
        pool = part if pool is None else pool + part
    hid_copy = pltpu.make_async_copy(hid, hid_hbm.at[0], load_sem.at[9])
    hid_copy.start()

    pooled = jnp.sum(pool, axis=0, keepdims=True) * gain_ref[...].reshape(1, D) * (1.0 / PATCHES)
    first = pooled.astype(BF16).astype(F32)
    rest = pooled - first
    second = rest.astype(BF16).astype(F32)
    third = rest - second
    at = lax.broadcasted_iota(jnp.int32, (16, D), 0)
    split = jnp.where(at == 0, first, jnp.where(at == 1, second, jnp.where(at == 2, third, 0.0))).astype(BF16)
    loads[5].wait()
    projected = jnp.sum(jnp.dot(split, wproj[...], preferred_element_type=F32)[0:8], axis=0, keepdims=True)
    for k in range(8):
        e_buf[s, k : k + 1, :] = projected[:, k * 128 : (k + 1) * 128]
    others(NSEQ, s, lambda p: e_copy(p, s).start())

    whole(o_send, NSEQ - 1, o_ss, o_rs).wait_send()
    label_row = labels_ref[...].reshape(1, NB)
    lane64 = lax.broadcasted_iota(jnp.int32, (1, 64), 1)
    own_label = jnp.sum(jnp.where(lane64 == b, label_row, 0), axis=1, keepdims=True)
    grid_i = lax.broadcasted_iota(jnp.int32, (64, 64), 0)
    grid_j = lax.broadcasted_iota(jnp.int32, (64, 64), 1)
    label_col = jnp.sum(
        jnp.where(grid_i == grid_j, jnp.broadcast_to(label_row, (64, 64)), 0), axis=1, keepdims=True
    )

    whole(tex, NB - NB1, t2_ss, t2_rs).wait_send()
    whole(tex, NB - NB1, t2_ss, t2_rs).wait_recv()
    whole(e_buf, NSEQ - 1, e_ss, e_rs).wait_recv()
    embedding = jnp.sum(e_buf[...], axis=0)
    squares = jnp.sum(jnp.sum(embedding * embedding, axis=0, keepdims=True), axis=1, keepdims=True)
    products = jnp.sum(tex[...] * embedding[None], axis=1)
    raw = jnp.sum(products.T, axis=0, keepdims=True)
    logits = raw * lax.rsqrt(squares + 1e-06)
    rows[b] = jnp.concatenate([logits, jnp.zeros((1, 64), F32)], axis=1)
    others(NB1, b_lo, lambda p: b1_copy(p, b_lo).start())

    peak = jnp.max(logits, axis=1, keepdims=True)
    lse = peak + jnp.log(jnp.sum(jnp.exp(logits - peak), axis=1, keepdims=True))
    chosen = jnp.sum(jnp.where(lane64 == own_label, logits, 0.0), axis=1, keepdims=True)
    image_loss = lse - chosen
    whole(e_buf, NSEQ - 1, e_ss, e_rs).wait_send()

    whole(rows, NB1 - 1, b1_ss, b1_rs).wait_recv()
    others(NB2, b_hi, lambda p: b2_copy(p, b_hi).start())
    whole(rows, NB1 - 1, b1_ss, b1_rs).wait_send()
    hid_copy.wait()
    whole(rows, NB - NB1, b2_ss, b2_rs).wait_recv()

    lane128 = lax.broadcasted_iota(jnp.int32, (64, 128), 1)
    column = jnp.sum(jnp.where(lane128 == b, rows[...].reshape(64, 128), 0.0), axis=1, keepdims=True)
    high = jnp.max(column, axis=0, keepdims=True)
    total = high + jnp.log(jnp.sum(jnp.exp(column - high), axis=0, keepdims=True))
    match = jnp.sum(jnp.where(label_col == b, column, 0.0), axis=0, keepdims=True)
    losses_ref[...] = jnp.where(lax.broadcasted_iota(jnp.int32, (1, 128), 1) == 0, image_loss, total - match)
    losses_copy = pltpu.make_async_copy(losses_ref, losses_hbm, load_sem.at[0])
    losses_copy.start()
    whole(rows, NB - NB1, b2_ss, b2_rs).wait_send()
    losses_copy.wait()


def hand_over(hid_hbm, losses_hbm, out_hbm, img_ref, txt_ref, held, scores, in_sem, out_sem):
    quarter = ROWS // 4
    cuts = [pl.ds(i * quarter, quarter) for i in range(4)]
    read = [pltpu.make_async_copy(hid_hbm.at[0, cut], held.at[cut], in_sem.at[i]) for i, cut in enumerate(cuts)]
    write = [pltpu.make_async_copy(held.at[cut], out_hbm.at[0, cut], out_sem.at[i]) for i, cut in enumerate(cuts)]
    numbers = pltpu.make_async_copy(losses_hbm, scores, in_sem.at[4])
    numbers.start()
    for r in read:
        r.start()
    for r, w in zip(read, write):
        r.wait()
        w.start()
    numbers.wait()
    img_ref[0] = scores[0, 0]
    txt_ref[0] = scores[0, 1]
    for w in write:
        w.wait()


def body(queries, keys, values, residual_in, w_out, ln_gain, w_proj, texts, labels):
    far_space = pl.BlockSpec(memory_space=pltpu.HBM)
    any_space = pl.BlockSpec(memory_space=pl.ANY)
    dma = pltpu.SemaphoreType.DMA
    hidden_out, losses = pl.pallas_call(
        kernel,
        out_shape=(
            jax.ShapeDtypeStruct((1, ROWS, D), BF16),
            jax.ShapeDtypeStruct((1, 128), F32),
        ),
        in_specs=[far_space] * 9,
        out_specs=(any_space, any_space),
        scratch_shapes=[
            pltpu.VMEM((ROWS, D), BF16),
            pltpu.VMEM((ROWS, D), BF16),
            pltpu.VMEM((ROWS, D), BF16),
            pltpu.VMEM((ROWS, D), BF16),
            pltpu.VMEM((D, D), BF16),
            pltpu.VMEM((D, EMBED), BF16),
            pltpu.VMEM((D,), F32),
            pltpu.VMEM((1, 64), F32),
            pltpu.VMEM((NB,), jnp.int32),
            pltpu.VMEM((ROWS, D), BF16),
            pltpu.VMEM((1, 128), F32),
            pltpu.VMEM((NSEQ, 2 * HD, ROWS), BF16),
            pltpu.VMEM((NSEQ, HD, ROWS), BF16),
            pltpu.VMEM((NSEQ, 2 * HD, ROWS), BF16),
            pltpu.VMEM((NSEQ, HD, ROWS), BF16),
            pltpu.VMEM((NSEQ, HD, ROWS), BF16),
            pltpu.VMEM((NSEQ, HD, ROWS), BF16),
            pltpu.VMEM((PATCHES, HD), BF16),
            pltpu.VMEM((HD + 16, PATCHES), BF16),
            pltpu.VMEM((PATCHES, CHUNK), F32),
            pltpu.VMEM((ROWS, D), F32),
            pltpu.VMEM((NSEQ, 1, 128), F32),
            pltpu.VMEM((NB, 8, 128), F32),
            pltpu.VMEM((NSEQ, 8, 128), F32),
            pltpu.VMEM((NB, 1, 128), F32),
            dma((10,)),
            dma((1,)), dma((NSEQ,)),
            dma((1,)), dma((NSEQ,)),
            dma((1,)), dma((NSEQ,)),
            dma((1,)), dma((1,)),
            dma((1,)), dma((1,)),
            dma((1,)), dma((1,)),
            dma((1,)), dma((1,)),
            dma((1,)), dma((1,)),
            dma((1,)), dma((1,)),
        ],
        compiler_params=pltpu.CompilerParams(
            collective_id=0, has_side_effects=True, vmem_limit_bytes=67043328
        ),
        name="attend_and_score",
    )(
        queries.reshape(ROWS, D),
        keys.reshape(ROWS, D),
        values.reshape(ROWS, D),
        residual_in.reshape(ROWS, D),
        w_out,
        ln_gain,
        w_proj,
        texts,
        labels,
    )
    smem = pl.BlockSpec(memory_space=pltpu.SMEM)
    return pl.pallas_call(
        hand_over,
        out_shape=(
            jax.ShapeDtypeStruct((1, ROWS, D), BF16),
            jax.ShapeDtypeStruct((1,), F32),
            jax.ShapeDtypeStruct((1,), F32),
        ),
        in_specs=[any_space] * 2,
        out_specs=(any_space, smem, smem),
        scratch_shapes=[pltpu.VMEM((ROWS, D), BF16), pltpu.SMEM((1, 128), F32), dma((5,)), dma((4,))],
        compiler_params=pltpu.CompilerParams(vmem_limit_bytes=67043328),
        name="hand_over",
    )(hidden_out, losses)


def solution(mesh):
    return jax.shard_map(
        body,
        mesh=mesh,
        in_specs=(
            P("batch", "seq", None),
            P("batch", "seq", None),
            P("batch", "seq", None),
            P("batch", "seq", None),
            P(),
            P(),
            P(),
            P("batch", "seq"),
            P(),
        ),
        out_specs=(P("batch", "seq", None), P("batch"), P("batch")),
        check_vma=False,
    )
```

```python
import math

import jax
import jax.numpy as jnp
from jax import lax
from jax.experimental import pallas as pl
from jax.experimental.pallas import tpu as pltpu
from jax.sharding import PartitionSpec as P

HEADS = 16
HD = 80
D = 1280
EMBED = 1024
PATCHES = 2048
ROWS = 128
NSEQ = 16
NZ = 8
NB = 64
NB1 = 16
NB2 = 4
CHUNK = 2 * ROWS
KB = 256
MESH = pl.DeviceIdType.MESH
F32 = jnp.float32
BF16 = jnp.bfloat16


def depth_step(t):
    half = (t + 1) // 2
    return lax.rem(4 + half * (1 - 2 * lax.rem(t, 2)) + NZ, NZ)


def kernel(
    q_hbm, k_hbm, v_hbm, res_hbm, wout_hbm, gain_hbm, wproj_hbm, texts_hbm, labels_hbm,
    hid_hbm, losses_hbm,
    q_in, k_in, v_in, res_in, wout, wproj, gain_ref, texts_ref, labels_ref, hid, losses_ref,
    kv_send, q_send, kv_recv, q_recv, o_send, o_recv,
    k_all, vt_all, s_all, acc, t0, tex, e_buf, rows,
    load_sem, kv_ss, kv_rs, q_ss, q_rs, o_ss, o_rs, t0_ss, t0_rs, t1_ss, t1_rs, t2_ss, t2_rs,
    e_ss, e_rs, b1_ss, b1_rs, b2_ss, b2_rs,
):
    b = lax.axis_index("batch")
    s = lax.axis_index("seq")
    z, y = s // 2, lax.rem(s, 2)
    b_hi, b_lo = b // NB1, lax.rem(b, NB1)

    loads = [
        pltpu.make_async_copy(src, dst, load_sem.at[i])
        for i, (src, dst) in enumerate(
            [
                (k_hbm, k_in),
                (v_hbm, v_in),
                (q_hbm, q_in),
                (res_hbm, res_in),
                (wout_hbm, wout),
                (wproj_hbm, wproj),
                (texts_hbm, texts_ref),
                (gain_hbm, gain_ref),
                (labels_hbm, labels_ref),
            ]
        )
    ]
    for i in (0, 1, 6, 2):
        loads[i].start()

    barrier = pltpu.get_barrier_semaphore()

    def greet_seq(r, c):
        pl.semaphore_signal(barrier, inc=1, device_id=(b, lax.rem(s + r, NSEQ)), device_id_type=MESH)
        pl.semaphore_signal(
            barrier, inc=1, device_id=(b_hi * NB1 + lax.rem(b_lo + r, NB1), s), device_id_type=MESH
        )
        return c

    lax.fori_loop(1, NSEQ, greet_seq, 0)

    def greet_far(r, c):
        pl.semaphore_signal(barrier, inc=1, device_id=(lax.rem(b + r * NB1, NB), s), device_id_type=MESH)
        return c

    lax.fori_loop(1, NB2, greet_far, 0)

    def turn(src, put):
        for c in range(D // 128):
            block = src[:, c * 128 : (c + 1) * 128].T
            i = 0
            while i < 8:
                g = c * 8 + i
                n = min(8 - i, 5 - g % 5)
                put(g // 5, (g % 5) * 16, block[i * 16 : (i + n) * 16], n * 16)
                i += n

    def put_k(h, r, value, n):
        kv_send[h, r : r + n, :] = value

    def put_v(h, r, value, n):
        kv_send[h, HD + r : HD + r + n, :] = value

    def put_q(h, r, value, n):
        q_send[h, r : r + n, :] = value

    loads[0].wait()
    turn(k_in, put_k)
    loads[1].wait()
    turn(v_in, put_v)
    for i in (3, 4, 5, 7, 8):
        loads[i].start()

    loads[6].wait()
    piece = texts_ref[...]
    blank = jnp.zeros((1, 64), F32)
    even = jnp.concatenate([piece, blank], axis=1)
    odd = jnp.concatenate([blank, piece], axis=1)
    t0[s] = jnp.where(y == 0, even, odd)

    pl.semaphore_wait(barrier, 2 * (NSEQ - 1) + NB2 - 1)

    def kv_copy(to, frm):
        return pltpu.make_async_remote_copy(
            src_ref=kv_send.at[to], dst_ref=kv_recv.at[frm], send_sem=kv_ss.at[0], recv_sem=kv_rs.at[frm],
            device_id=(b, to), device_id_type=MESH,
        )

    def q_copy(to, frm):
        return pltpu.make_async_remote_copy(
            src_ref=q_send.at[to], dst_ref=q_recv.at[frm], send_sem=q_ss.at[0], recv_sem=q_rs.at[frm],
            device_id=(b, to), device_id_type=MESH,
        )

    def o_copy(to, frm):
        return pltpu.make_async_remote_copy(
            src_ref=o_send.at[to], dst_ref=o_recv.at[frm], send_sem=o_ss.at[0], recv_sem=o_rs.at[frm],
            device_id=(b, to), device_id_type=MESH,
        )

    def t0_copy(to, frm):
        return pltpu.make_async_remote_copy(
            src_ref=t0.at[frm], dst_ref=t0.at[frm], send_sem=t0_ss.at[0], recv_sem=t0_rs.at[0],
            device_id=(b, to), device_id_type=MESH,
        )

    def e_copy(to, frm):
        return pltpu.make_async_remote_copy(
            src_ref=e_buf.at[frm], dst_ref=e_buf.at[frm], send_sem=e_ss.at[0], recv_sem=e_rs.at[0],
            device_id=(b, to), device_id_type=MESH,
        )

    def t1_copy(to, frm):
        at = b_hi * NB1 + frm
        return pltpu.make_async_remote_copy(
            src_ref=tex.at[at], dst_ref=tex.at[at], send_sem=t1_ss.at[0], recv_sem=t1_rs.at[0],
            device_id=(b_hi * NB1 + to, s), device_id_type=MESH,
        )

    def b1_copy(to, frm):
        at = b_hi * NB1 + frm
        return pltpu.make_async_remote_copy(
            src_ref=rows.at[at], dst_ref=rows.at[at], send_sem=b1_ss.at[0], recv_sem=b1_rs.at[0],
            device_id=(b_hi * NB1 + to, s), device_id_type=MESH,
        )

    def t2_copy(to, frm):
        at = pl.ds(frm * NB1, NB1)
        return pltpu.make_async_remote_copy(
            src_ref=tex.at[at], dst_ref=tex.at[at], send_sem=t2_ss.at[0], recv_sem=t2_rs.at[0],
            device_id=(to * NB1 + b_lo, s), device_id_type=MESH,
        )

    def b2_copy(to, frm):
        at = pl.ds(frm * NB1, NB1)
        return pltpu.make_async_remote_copy(
            src_ref=rows.at[at], dst_ref=rows.at[at], send_sem=b2_ss.at[0], recv_sem=b2_rs.at[0],
            device_id=(to * NB1 + b_lo, s), device_id_type=MESH,
        )

    def whole(ref, count, send_sem, recv_sem):
        part = ref.at[pl.ds(0, count)]
        return pltpu.make_async_remote_copy(
            src_ref=part, dst_ref=part, send_sem=send_sem.at[0], recv_sem=recv_sem.at[0],
            device_id=(b, lax.rem(s + 1, NSEQ)), device_id_type=MESH,
        )

    def others(count, me, act):
        def step(r, c):
            act(lax.rem(me + r, count))
            return c

        lax.fori_loop(1, count, step, 0)

    def by_depth(sign, act):
        def step(t, c):
            there = lax.rem(z + sign * depth_step(NZ - 1 - t) + NZ, NZ)
            for w in range(2):
                peer = 2 * there + lax.rem(y + w, 2)

                @pl.when(peer != s)
                def _():
                    act(peer)

            return c

        lax.fori_loop(0, NZ, step, 0)

    others(NSEQ, s, lambda p: t0_copy(p, s).start())
    by_depth(1, lambda p: kv_copy(p, s).start())

    loads[2].wait()
    turn(q_in, put_q)
    by_depth(1, lambda p: q_copy(p, s).start())

    kv_recv[s] = kv_send[s]
    q_recv[s] = q_send[s]
    top = lax.broadcasted_iota(jnp.int32, (16, PATCHES), 0)
    vt_all[HD : HD + 16, :] = jnp.where(top == 0, 1.0, 0.0).astype(BF16)

    def take_kv(t, c):
        there = lax.rem(z - depth_step(NZ - 1 - t) + NZ, NZ)
        for w in range(2):
            peer = 2 * there + w

            @pl.when(peer != s)
            def _():
                kv_copy(s, peer).wait_recv()

            block = kv_recv[peer]
            k_all[pl.ds(pl.multiple_of((2 * t + w) * ROWS, ROWS), ROWS), :] = block[:HD].T
            vt_all[0:HD, pl.ds(pl.multiple_of((2 * t + w) * ROWS, ROWS), ROWS)] = block[HD:]
        return c

    lax.fori_loop(0, NZ, take_kv, 0)

    whole(t0, NSEQ - 1, t0_ss, t0_rs).wait_recv()
    for k in range(8):
        tex[b, k : k + 1, :] = t0[2 * k] + t0[2 * k + 1]
    others(NB1, b_lo, lambda p: t1_copy(p, b_lo).start())

    loads[3].wait()
    acc[...] = res_in[...].astype(F32)
    factor = HD ** (-0.5) * math.log2(math.e)

    def attend(t, c):
        @pl.when(t == 2)
        def _():
            whole(tex, NB1 - 1, t1_ss, t1_rs).wait_recv()
            others(NB2, b_hi, lambda p: t2_copy(p, b_hi).start())

        depths = [lax.rem(z - depth_step(2 * t + u) + NZ, NZ) for u in range(2)]
        for there in depths:
            for w in range(2):
                peer = 2 * there + w

                @pl.when(peer != s)
                def _():
                    q_copy(s, peer).wait_recv()

        maxima = []
        for u, there in enumerate(depths):
            qt = jnp.concatenate([q_recv[2 * there], q_recv[2 * there + 1]], axis=1)
            top8 = None
            for i in range(PATCHES // KB):
                part = jnp.dot(k_all[i * KB : (i + 1) * KB, :], qt, preferred_element_type=F32)
                s_all[u, i * KB : (i + 1) * KB, :] = part
                high = jnp.max(part.reshape(KB // 8, 8, CHUNK), axis=0)
                top8 = high if top8 is None else jnp.maximum(top8, high)
            maxima.append(jnp.max(top8, axis=0, keepdims=True))
        mixed = []
        for u in range(2):
            total = None
            for i in range(PATCHES // KB):
                weights = jnp.exp2((s_all[u, i * KB : (i + 1) * KB, :] - maxima[u]) * factor).astype(BF16)
                part = jnp.dot(vt_all[:, i * KB : (i + 1) * KB], weights, preferred_element_type=F32)
                total = part if total is None else total + part
            mixed.append((total[:HD] / total[HD : HD + 1]).astype(BF16))
        for u, there in enumerate(depths):
            for w in range(2):
                peer = 2 * there + w
                value = mixed[u][:, w * ROWS : (w + 1) * ROWS]

                @pl.when(peer != s)
                def _():
                    o_send[peer] = value
                    o_copy(peer, s).start()

                @pl.when(peer == s)
                def _():
                    o_recv[s] = value

        return c

    lax.fori_loop(0, NZ // 2, attend, 0)

    whole(kv_send, NSEQ - 1, kv_ss, kv_rs).wait_send()
    whole(q_send, NSEQ - 1, q_ss, q_rs).wait_send()
    whole(t0, NSEQ - 1, t0_ss, t0_rs).wait_send()
    whole(tex, NB1 - 1, t1_ss, t1_rs).wait_send()

    loads[4].wait()
    loads[7].wait()
    loads[8].wait()

    def project(t, c):
        there = lax.rem(z + depth_step(t) + NZ, NZ)
        for w in range(2):
            peer = 2 * there + w

            @pl.when(peer != s)
            def _():
                o_copy(s, peer).wait_recv()

        part = jnp.concatenate([o_recv[2 * there], o_recv[2 * there + 1]], axis=0).T
        weight = wout[pl.ds(pl.multiple_of(there * 2 * HD, 2 * HD), 2 * HD), :]
        acc[...] += jnp.dot(part, weight, preferred_element_type=F32)
        return c

    lax.fori_loop(0, NZ, project, 0)

    pool = None
    for i in range(ROWS // 16):
        x = acc[i * 16 : (i + 1) * 16, :]
        hid[i * 16 : (i + 1) * 16, :] = x.astype(BF16)
        centred = x - jnp.sum(x, axis=1, keepdims=True) * (1.0 / D)
        variance = jnp.sum(centred * centred, axis=1, keepdims=True) * (1.0 / D)
        normed = (centred * lax.rsqrt(variance + 1e-05)).reshape(2, 8, D)
        part = normed[0] + normed[1]
        pool = part if pool is None else pool + part
    hid_copy = pltpu.make_async_copy(hid, hid_hbm.at[0], load_sem.at[9])
    hid_copy.start()

    pooled = jnp.sum(pool, axis=0, keepdims=True) * gain_ref[...].reshape(1, D) * (1.0 / PATCHES)
    first = pooled.astype(BF16).astype(F32)
    rest = pooled - first
    second = rest.astype(BF16).astype(F32)
    third = rest - second
    at = lax.broadcasted_iota(jnp.int32, (16, D), 0)
    split = jnp.where(at == 0, first, jnp.where(at == 1, second, jnp.where(at == 2, third, 0.0))).astype(BF16)
    loads[5].wait()
    projected = jnp.sum(jnp.dot(split, wproj[...], preferred_element_type=F32)[0:8], axis=0, keepdims=True)
    for k in range(8):
        e_buf[s, k : k + 1, :] = projected[:, k * 128 : (k + 1) * 128]
    others(NSEQ, s, lambda p: e_copy(p, s).start())

    whole(o_send, NSEQ - 1, o_ss, o_rs).wait_send()
    label_row = labels_ref[...].reshape(1, NB)
    lane64 = lax.broadcasted_iota(jnp.int32, (1, 64), 1)
    own_label = jnp.sum(jnp.where(lane64 == b, label_row, 0), axis=1, keepdims=True)
    grid_i = lax.broadcasted_iota(jnp.int32, (64, 64), 0)
    grid_j = lax.broadcasted_iota(jnp.int32, (64, 64), 1)
    label_col = jnp.sum(
        jnp.where(grid_i == grid_j, jnp.broadcast_to(label_row, (64, 64)), 0), axis=1, keepdims=True
    )

    whole(tex, NB - NB1, t2_ss, t2_rs).wait_send()
    whole(tex, NB - NB1, t2_ss, t2_rs).wait_recv()
    whole(e_buf, NSEQ - 1, e_ss, e_rs).wait_recv()
    embedding = jnp.sum(e_buf[...], axis=0)
    squares = jnp.sum(jnp.sum(embedding * embedding, axis=0, keepdims=True), axis=1, keepdims=True)
    products = jnp.sum(tex[...] * embedding[None], axis=1)
    raw = jnp.sum(products.T, axis=0, keepdims=True)
    logits = raw * lax.rsqrt(squares + 1e-06)
    rows[b] = jnp.concatenate([logits, jnp.zeros((1, 64), F32)], axis=1)
    others(NB1, b_lo, lambda p: b1_copy(p, b_lo).start())

    peak = jnp.max(logits, axis=1, keepdims=True)
    lse = peak + jnp.log(jnp.sum(jnp.exp(logits - peak), axis=1, keepdims=True))
    chosen = jnp.sum(jnp.where(lane64 == own_label, logits, 0.0), axis=1, keepdims=True)
    image_loss = lse - chosen
    whole(e_buf, NSEQ - 1, e_ss, e_rs).wait_send()

    whole(rows, NB1 - 1, b1_ss, b1_rs).wait_recv()
    others(NB2, b_hi, lambda p: b2_copy(p, b_hi).start())
    whole(rows, NB1 - 1, b1_ss, b1_rs).wait_send()
    hid_copy.wait()
    whole(rows, NB - NB1, b2_ss, b2_rs).wait_recv()

    lane128 = lax.broadcasted_iota(jnp.int32, (64, 128), 1)
    column = jnp.sum(jnp.where(lane128 == b, rows[...].reshape(64, 128), 0.0), axis=1, keepdims=True)
    high = jnp.max(column, axis=0, keepdims=True)
    total = high + jnp.log(jnp.sum(jnp.exp(column - high), axis=0, keepdims=True))
    match = jnp.sum(jnp.where(label_col == b, column, 0.0), axis=0, keepdims=True)
    losses_ref[...] = jnp.where(lax.broadcasted_iota(jnp.int32, (1, 128), 1) == 0, image_loss, total - match)
    losses_copy = pltpu.make_async_copy(losses_ref, losses_hbm, load_sem.at[0])
    losses_copy.start()
    whole(rows, NB - NB1, b2_ss, b2_rs).wait_send()
    losses_copy.wait()


def hand_over(hid_hbm, losses_hbm, out_hbm, img_ref, txt_ref, held, scores, in_sem, out_sem):
    quarter = ROWS // 4
    cuts = [pl.ds(i * quarter, quarter) for i in range(4)]
    read = [pltpu.make_async_copy(hid_hbm.at[0, cut], held.at[cut], in_sem.at[i]) for i, cut in enumerate(cuts)]
    write = [pltpu.make_async_copy(held.at[cut], out_hbm.at[0, cut], out_sem.at[i]) for i, cut in enumerate(cuts)]
    numbers = pltpu.make_async_copy(losses_hbm, scores, in_sem.at[4])
    numbers.start()
    for r in read:
        r.start()
    for r, w in zip(read, write):
        r.wait()
        w.start()
    numbers.wait()
    img_ref[0] = scores[0, 0]
    txt_ref[0] = scores[0, 1]
    for w in write:
        w.wait()


def body(queries, keys, values, residual_in, w_out, ln_gain, w_proj, texts, labels):
    far_space = pl.BlockSpec(memory_space=pltpu.HBM)
    any_space = pl.BlockSpec(memory_space=pl.ANY)
    dma = pltpu.SemaphoreType.DMA
    hidden_out, losses = pl.pallas_call(
        kernel,
        out_shape=(
            jax.ShapeDtypeStruct((1, ROWS, D), BF16),
            jax.ShapeDtypeStruct((1, 128), F32),
        ),
        in_specs=[far_space] * 9,
        out_specs=(any_space, any_space),
        scratch_shapes=[
            pltpu.VMEM((ROWS, D), BF16),
            pltpu.VMEM((ROWS, D), BF16),
            pltpu.VMEM((ROWS, D), BF16),
            pltpu.VMEM((ROWS, D), BF16),
            pltpu.VMEM((D, D), BF16),
            pltpu.VMEM((D, EMBED), BF16),
            pltpu.VMEM((D,), F32),
            pltpu.VMEM((1, 64), F32),
            pltpu.VMEM((NB,), jnp.int32),
            pltpu.VMEM((ROWS, D), BF16),
            pltpu.VMEM((1, 128), F32),
            pltpu.VMEM((NSEQ, 2 * HD, ROWS), BF16),
            pltpu.VMEM((NSEQ, HD, ROWS), BF16),
            pltpu.VMEM((NSEQ, 2 * HD, ROWS), BF16),
            pltpu.VMEM((NSEQ, HD, ROWS), BF16),
            pltpu.VMEM((NSEQ, HD, ROWS), BF16),
            pltpu.VMEM((NSEQ, HD, ROWS), BF16),
            pltpu.VMEM((PATCHES, HD), BF16),
            pltpu.VMEM((HD + 16, PATCHES), BF16),
            pltpu.VMEM((2, PATCHES, CHUNK), F32),
            pltpu.VMEM((ROWS, D), F32),
            pltpu.VMEM((NSEQ, 1, 128), F32),
            pltpu.VMEM((NB, 8, 128), F32),
            pltpu.VMEM((NSEQ, 8, 128), F32),
            pltpu.VMEM((NB, 1, 128), F32),
            dma((10,)),
            dma((1,)), dma((NSEQ,)),
            dma((1,)), dma((NSEQ,)),
            dma((1,)), dma((NSEQ,)),
            dma((1,)), dma((1,)),
            dma((1,)), dma((1,)),
            dma((1,)), dma((1,)),
            dma((1,)), dma((1,)),
            dma((1,)), dma((1,)),
            dma((1,)), dma((1,)),
        ],
        compiler_params=pltpu.CompilerParams(
            collective_id=0, has_side_effects=True, vmem_limit_bytes=67043328
        ),
        name="attend_and_score",
    )(
        queries.reshape(ROWS, D),
        keys.reshape(ROWS, D),
        values.reshape(ROWS, D),
        residual_in.reshape(ROWS, D),
        w_out,
        ln_gain,
        w_proj,
        texts,
        labels,
    )
    smem = pl.BlockSpec(memory_space=pltpu.SMEM)
    return pl.pallas_call(
        hand_over,
        out_shape=(
            jax.ShapeDtypeStruct((1, ROWS, D), BF16),
            jax.ShapeDtypeStruct((1,), F32),
            jax.ShapeDtypeStruct((1,), F32),
        ),
        in_specs=[any_space] * 2,
        out_specs=(any_space, smem, smem),
        scratch_shapes=[pltpu.VMEM((ROWS, D), BF16), pltpu.SMEM((1, 128), F32), dma((5,)), dma((4,))],
        compiler_params=pltpu.CompilerParams(vmem_limit_bytes=67043328),
        name="hand_over",
    )(hidden_out, losses)


def solution(mesh):
    return jax.shard_map(
        body,
        mesh=mesh,
        in_specs=(
            P("batch", "seq", None),
            P("batch", "seq", None),
            P("batch", "seq", None),
            P("batch", "seq", None),
            P(),
            P(),
            P(),
            P("batch", "seq"),
            P(),
        ),
        out_specs=(P("batch", "seq", None), P("batch"), P("batch")),
        check_vma=False,
    )
```
